128 devices in a mesh: member: 8 (over x, core), region: 16 (over z, y).
Axes of the slice: x: 4, y: 4, z: 4, core: 2. Of those that a mesh axis runs over, the one named last changes fastest.
Arguments:
- ensemble: float32 [24, 32, 128, 512], P('member', 'region'), may hold values from -6 to 6
- obs_value: float32 [32, 128, 128], P(None, ('member', 'region')), may hold values from -6 to 6
- obs_error: float32 [32, 128, 128], P(None, ('member', 'region')), may hold values from 0.5 to 4
- obs_index: int32 [32, 128, 128], P(None, ('member', 'region')), may hold values from 0 to 511
- obs_count: int32 [32, 128], P(None, ('member', 'region')), may hold values from 1 to 128
Outputs:
- analysis: float32 [24, 32, 128, 512], P('member', 'region')
The draws below stay inside these ranges and needn't reach their ends.
Inputs may be any that keep to these rules, and one draw needn't show every extreme that they name: `obs_index`: value v names field v // (256) (0 SST, 1 SSH) at cell v mod (256) of the block, cells row-major. `obs_count`: slots below a block's count are observations; the others are padding and carry no weight.
All inputs are finite; a program needn't handle non-finite values.
Results may differ from the reference program's by a relative error of at most 0.0001.
Values sent between devices are 32-bit elements; how exact they have to be, the bound alone decides.
A program may use at most 64 MiB of HBM per device.

```python
import math
import jax
import jax.numpy as jnp
from jax import lax

SIDE = 16
OBS = 128
NS_ITERS = 6
VALS = 512
MEMBERS = 24
BROWS = 32
BCOLS = 128


def set_ends(values, own_key, low, high):
    shape = values.shape
    place = [jax.random.randint(jax.random.fold_in(own_key, axis), (), 0, shape[axis]) for axis in range(len(shape))]
    values = values.at[tuple(place)].set(low)
    longest = shape.index(max(shape))
    place[longest] = (place[longest] + 1) % shape[longest]
    return values.at[tuple(place)].set(high)


def steps_of(key, extent, cuts, smallest, top_value):
    def one(dim, shards_of):
        draws = jax.random.uniform(jax.random.fold_in(jax.random.fold_in(key, 6), dim), (shards_of,), jnp.float32, smallest / len(cuts), top_value / len(cuts))
        return jnp.repeat(jnp.exp(draws), extent[dim] // shards_of).reshape((-1,) + (1,) * (len(extent) - dim - 1))

    loudness = one(*cuts[0])
    for cut in cuts[1:]:
        loudness = loudness * one(*cut)
    return loudness


def normal_values(key, shape, width, bound, shards=(), kind=jnp.bfloat16):
    result = jax.random.normal(key, shape, jnp.float32) * width
    if len(shards) > 0:
        result = steps_of(key, shape, shards, -0.22, 0.18) * result
    return jnp.clip(result, min=-bound, max=bound).astype(kind)


def setup_inputs(seed: int = 0) -> dict:
    streams_of = jax.random.split(jax.random.key(seed), 6)
    ensemble = normal_values(streams_of[0], (MEMBERS, BROWS, BCOLS, VALS), 1.0, 6.0, ((0, 8), (1, 16)), jnp.float32)
    obs_value = normal_values(streams_of[1], (BROWS, BCOLS, OBS), 1.0, 6.0, ((1, 128),), jnp.float32)
    obs_error = jnp.clip(jnp.exp(math.log(4.0) - 2.0794415 * jax.random.uniform(streams_of[2], (BROWS, BCOLS, OBS), jnp.float32) ** steps_of(streams_of[2], (BROWS, BCOLS, OBS), ((1, 128),), -0.2, 0.2)), 0.5, 4.0)
    obs_index = set_ends(jax.random.randint(streams_of[3], (BROWS, BCOLS, OBS), 0, VALS), jax.random.fold_in(streams_of[3], 1), 0, VALS - 1).astype(jnp.int32)
    obs_count = set_ends(jax.random.randint(streams_of[4], (BROWS, BCOLS), 1, OBS + 1), jax.random.fold_in(streams_of[4], 1), 1, OBS).astype(jnp.int32)
    return dict(ensemble=ensemble, obs_value=obs_value, obs_error=obs_error, obs_index=obs_index, obs_count=obs_count)


LOC_SCALE = 12.0
INFLATION_FACTOR = 1.1

def batch_product(left, right):
    return jnp.einsum('...ij,...jk->...ik', left, right, precision=lax.Precision.HIGHEST)

def observe(ensemble, obs_value, obs_error, obs_index, obs_count):
    ens_mean = lax.optimization_barrier(jnp.mean(ensemble, axis=0))
    anomaly = ensemble - ens_mean
    slot_index = lax.broadcasted_iota(jnp.int32, obs_index.shape, 2)
    live_slot = jnp.where(slot_index < obs_count[:, :, None], 1.0, 0.0).astype(jnp.float32)
    root_weight = jnp.sqrt(live_slot / obs_error)
    full_index = jnp.broadcast_to(obs_index[None], (anomaly.shape[0],) + obs_index.shape).astype(jnp.int32)
    seen_anom = jnp.take_along_axis(anomaly, full_index, axis=3)
    seen_mean = jnp.take_along_axis(ens_mean, obs_index.astype(jnp.int32), axis=2)
    rescaled_values = root_weight[:, :, None] * jnp.moveaxis(seen_anom, 0, 2)
    innovation = root_weight * (obs_value - seen_mean)
    cell_index = obs_index % (SIDE * SIDE)
    rowpos = (cell_index // SIDE).astype(jnp.float32)
    column_position = (cell_index % SIDE).astype(jnp.float32)
    stacked = jnp.concatenate([rescaled_values, innovation[:, :, None], rowpos[:, :, None], column_position[:, :, None]], axis=2)
    return (anomaly, ens_mean, stacked)

def analyze(anomaly, ens_mean, padded):
    ensemble_members = anomaly.shape[0]
    row_count = anomaly.shape[1]
    col_count = anomaly.shape[2]
    pieces = []
    for row_step in range(3):
        for col_step in range(3):
            pieces.append(padded[row_step:row_step + row_count, col_step:col_step + col_count])
    nearby = jnp.stack(pieces, axis=2)
    rescaled_values = nearby[:, :, :, :ensemble_members]
    innovation = nearby[:, :, :, ensemble_members]
    rowpos = nearby[:, :, :, ensemble_members + 1]
    column_position = nearby[:, :, :, ensemble_members + 2]
    offset_index = jnp.arange(9, dtype=jnp.int32)
    offset_row = (offset_index // 3 - 1).astype(jnp.float32) * SIDE
    offset_col = (offset_index % 3 - 1).astype(jnp.float32) * SIDE
    half_side = SIDE // 2
    point_index = jnp.arange(4, dtype=jnp.int32)
    center_row = (point_index // 2).astype(jnp.float32) * half_side + (half_side - 1) * 0.5
    center_col = (point_index % 2).astype(jnp.float32) * half_side + (half_side - 1) * 0.5
    row_gap = offset_row[:, None] + rowpos
    col_gap = offset_col[:, None] + column_position
    distance = (row_gap[:, :, None] - center_row[:, None, None]) ** 2 + (col_gap[:, :, None] - center_col[:, None, None]) ** 2
    locality = jnp.exp(-distance / (2.0 * LOC_SCALE * LOC_SCALE))
    weighted = locality[:, :, :, :, None, :] * rescaled_values[:, :, None]
    gramian_total = jnp.einsum('rcpnko,rcnjo->rcpkj', weighted, rescaled_values, precision=lax.Precision.HIGHEST)
    drive_vec = jnp.einsum('rcpnko,rcno->rcpk', weighted, innovation, precision=lax.Precision.HIGHEST)
    identity_matrix = jnp.eye(ensemble_members, dtype=jnp.float32)
    precision_matrix = gramian_total + (ensemble_members - 1) / INFLATION_FACTOR * identity_matrix
    norm_scale = jnp.sqrt(lax.optimization_barrier(jnp.sum(precision_matrix * precision_matrix, axis=(3, 4), keepdims=True)))
    root_iter = precision_matrix / norm_scale
    inv_iter = jnp.broadcast_to(identity_matrix, precision_matrix.shape)
    for sweep_index in range(NS_ITERS):
        ns_step = 1.5 * identity_matrix - 0.5 * batch_product(inv_iter, root_iter)
        root_iter = batch_product(root_iter, ns_step)
        inv_iter = batch_product(ns_step, inv_iter)
    inv_root = inv_iter / jnp.sqrt(norm_scale)
    half_way = jnp.einsum('rcpkj,rcpj->rcpk', inv_root, drive_vec, precision=lax.Precision.HIGHEST)
    mean_w = jnp.einsum('rcpkj,rcpj->rcpk', inv_root, half_way, precision=lax.Precision.HIGHEST)
    weights = mean_w[..., :, None] + math.sqrt(ensemble_members - 1) * inv_root
    point_weights = weights.reshape(row_count, col_count, 2, 2, ensemble_members, ensemble_members)
    shaped = anomaly.reshape(ensemble_members, row_count, col_count, 2, 2, half_side, 2, half_side)
    updated = jnp.einsum('jrcvaybx,rcabjk->krcvaybx', shaped, point_weights, precision=lax.Precision.HIGHEST)
    return ens_mean[None] + updated.reshape(anomaly.shape)

def reference(ensemble, obs_value, obs_error, obs_index, obs_count):
    anomaly, ens_mean, stacked = observe(ensemble, obs_value, obs_error, obs_index, obs_count)
    padded = jnp.pad(stacked, ((1, 1), (1, 1), (0, 0), (0, 0)))

    def one_row(row_index):
        part_anom = lax.dynamic_slice_in_dim(anomaly, row_index, 1, 1)
        part_mean = lax.dynamic_slice_in_dim(ens_mean, row_index, 1, 0)
        part_pad = lax.dynamic_slice_in_dim(padded, row_index, 3, 0)
        return analyze(part_anom, part_mean, part_pad)
    row_results = lax.map(one_row, jnp.arange(BROWS, dtype=jnp.int32))
    return jnp.moveaxis(row_results[:, :, 0], 0, 1)
```

```python
import functools
import math

import jax
import jax.numpy as jnp
from jax import lax
from jax.experimental import pallas as pl
from jax.experimental.pallas import tpu as pltpu
from jax.sharding import PartitionSpec as P

SIDE = 16
CELLS = SIDE * SIDE
HALF = SIDE // 2
LANES = 128
SUB = 8
NS_ITERS = 6
LOC_SCALE = 12.0
INFLATION_FACTOR = 1.1
MESH = pl.DeviceIdType.MESH
NT = (((1,), (1,)), ((), ()))
T = 8
PHASES = 2
OWN = 128
ROW_HALO = 32
SIDE_HALO = 16
TARGETS = 256


def split(values):
    high = values.astype(jnp.bfloat16)
    low = (values - high.astype(jnp.float32)).astype(jnp.bfloat16)
    return high, low


def row_of(k, jb):
    kb = k // SUB
    return (0, 192, 320)[kb] + (k - SUB * kb) * (24 - SUB * kb) + SUB * (jb - kb)


def kernel(
    dims,
    ens_ref, value_any, error_any, index_any, count_ref, out_ref,
    value_ref, error_ref, index_ref, ens, pack, obs, slots, place, lochi, loclo, qhi, qlo, own, hin,
    halo_out, row_in, side_in, root, inv, step, drv, half_ref, wt, xt, mean, outgoing,
    ens_send, ens_recv, obs_send, obs_recv, halo_send, halo_recv, out_send, out_recv, local_sem, own_sem,
):
    M, G, K, R, V, O = dims
    members = M * K
    blocks = members // SUB
    PACKED = own.shape[0]
    m = lax.axis_index("member")
    g = lax.axis_index("region")
    f32 = jnp.float32

    loads = []
    for n, (src, dst) in enumerate(((value_any, value_ref), (error_any, error_ref), (index_any, index_ref))):
        load = pltpu.make_async_copy(src, dst, local_sem.at[n])
        load.start()
        loads.append(load)

    def tile(p, d):
        return pl.ds(pl.multiple_of((p * M + d) * T, T), T)

    def own_copy(p):
        return pltpu.make_async_copy(
            ens_ref.at[:, :, tile(p, m), :], ens.at[p, pl.ds(m * K, K)], own_sem.at[p]
        )

    for p in range(PHASES):
        own_copy(p).start()

    column = m * G + g
    col_tile = column // T
    col_owner = lax.rem(col_tile, M)
    col_phase = col_tile // M
    col_at = lax.rem(column, T)
    holders = []
    for s in range(PHASES * T):
        c = ((s // T) * M + m) * T + s % T
        holders.append((c // G, lax.rem(c, G)))

    barrier = pltpu.get_barrier_semaphore()
    for off in range(1, M):
        pl.semaphore_signal(barrier, inc=1, device_id=(lax.rem(m + off, M), g), device_id_type=MESH)
    for hm, hg in holders:
        @pl.when(jnp.logical_not(jnp.logical_and(hm == m, hg == g)))
        def _():
            pl.semaphore_signal(barrier, inc=1, device_id=(hm, hg), device_id_type=MESH)
    up_ok = g > 0
    down_ok = g < G - 1
    row_ok = {-1: up_ok, 1: down_ok}
    for dg in (-1, 1):
        for dm in (-1, 0, 1):
            @pl.when(row_ok[dg])
            def _():
                pl.semaphore_signal(barrier, inc=1, device_id=(lax.rem(m + M + dm, M), g + dg), device_id_type=MESH)

    for load in loads:
        load.wait()
    slot = lax.broadcasted_iota(jnp.int32, (G * R, O), 1)
    slot_row = lax.broadcasted_iota(jnp.int32, (G * R, O), 0)
    count = jnp.zeros((G * R, O), jnp.int32)
    for d in range(G * R):
        count = jnp.where(slot_row == d, count_ref[0, d], count)
    live = jnp.where(slot < count, 1.0, 0.0).astype(f32)
    weight = jnp.sqrt(live / error_ref[...])
    value = value_ref[...]
    index_f = index_ref[...].astype(f32)
    for d in range(G):
        base = d * SUB
        pack[base : base + R, :] = weight[d * R : (d + 1) * R]
        pack[base + R : base + 2 * R, :] = value[d * R : (d + 1) * R]
        pack[base + 2 * R : base + 3 * R, :] = index_f[d * R : (d + 1) * R]
        pack[base + 3 * R : base + SUB, :] = jnp.zeros((SUB - 3 * R, O), f32)
    used = OWN + 2 * ROW_HALO
    lochi[used:, :] = jnp.zeros((TARGETS - used, lochi.shape[1]), jnp.bfloat16)
    loclo[used:, :] = jnp.zeros((TARGETS - used, lochi.shape[1]), jnp.bfloat16)

    ends = jnp.where(up_ok, 1, 0) + jnp.where(down_ok, 1, 0)
    self_obs = jnp.where(col_owner == m, 1, 0)
    pl.semaphore_wait(barrier, M - 1 + G - self_obs + 3 * ends)

    pieces = ((0, 1), (1, K))

    def ens_copy(p, n, off, to, at):
        a, b = pieces[n]
        return pltpu.make_async_remote_copy(
            src_ref=ens_ref.at[a:b, :, tile(p, to), :],
            dst_ref=ens.at[p, pl.ds(at * K + a, b - a)],
            send_sem=ens_send.at[p, n, off], recv_sem=ens_recv.at[p, n, off],
            device_id=(to, g), device_id_type=MESH,
        )

    def obs_copy(to_m, to_g, src_g, p, e):
        return pltpu.make_async_remote_copy(
            src_ref=pack.at[pl.ds(pl.multiple_of(src_g * SUB, SUB), SUB)],
            dst_ref=obs.at[p, pl.ds(pl.multiple_of(e * SUB, SUB), SUB)],
            send_sem=obs_send.at[src_g], recv_sem=obs_recv.at[p, e],
            device_id=(to_m, to_g), device_id_type=MESH,
        )

    for off in range(1, G):
        to = lax.rem(g + off, G)
        obs_copy(col_owner, to, to, col_phase, col_at).start()

    @pl.when(col_owner != m)
    def _():
        obs_copy(col_owner, g, g, col_phase, col_at).start()

    @pl.when(col_owner == m)
    def _():
        obs[col_phase, pl.ds(pl.multiple_of(col_at * SUB, SUB), SUB), :] = pack[
            pl.ds(pl.multiple_of(g * SUB, SUB), SUB), :
        ]

    order = [4, 5, 3, 2, 6, 1, 7]
    order = [off for off in order if off < M] + [off for off in range(1, M) if off not in order]
    for n in range(2):
        for off in order:
            ens_copy(0, n, off, lax.rem(m + off, M), m).start()
    for off in order:
        ens_copy(1, 0, off, lax.rem(m + off, M), m).start()
    for off in order:
        to = lax.rem(m + off, M)
        @pl.when(to == 0)
        def _():
            ens_copy(1, 1, off, to, m).start()

    for s, (hm, hg) in enumerate(holders):
        @pl.when(jnp.logical_not(jnp.logical_and(hm == m, hg == g)))
        def _():
            obs_copy(hm, hg, g, s // T, s % T).wait_recv()

    def wait_ens(p):
        own_copy(p).wait()
        for n in range(2):
            for off in range(1, M):
                came = lax.rem(m + M - off, M)
                ens_copy(p, n, off, came, came).wait_recv()

    tiles = V // LANES

    def gather(p):
        for i in range(R):
            wgt = obs[p, pl.ds(i, T, stride=SUB), :]
            val = obs[p, pl.ds(R + i, T, stride=SUB), :]
            idx = obs[p, pl.ds(2 * R + i, T, stride=SUB), :].astype(jnp.int32)
            lane = idx & (LANES - 1)
            which = idx >> 7
            cell = idx & (CELLS - 1)
            place[2 * i] = (cell >> 4).astype(f32)
            place[2 * i + 1] = (cell & (SIDE - 1)).astype(f32)
            seen = []
            for k in range(members):
                got = jnp.take_along_axis(ens[p, k, i, :, :LANES], lane, axis=1)
                for t in range(1, tiles):
                    more = jnp.take_along_axis(ens[p, k, i, :, t * LANES : (t + 1) * LANES], lane, axis=1)
                    got = jnp.where(which == t, more, got)
                seen.append(got)
            total = seen[0]
            for k in range(1, members):
                total = total + seen[k]
            avg = total * (1.0 / members)
            for k in range(members):
                slots[i, k * T : (k + 1) * T, :] = wgt * (seen[k] - avg)
            slots[i, members * T : (members + 1) * T, :] = wgt * (val - avg)

    sub8 = lax.broadcasted_iota(jnp.int32, (SUB, O), 0)

    def products(c, i):
        at = (c * R + i) * O
        here = [slots[i, pl.ds(c + b * SUB * T, SUB, stride=T), :] for b in range(blocks)]
        innov = slots[i, members * T + c : members * T + c + 1, :]
        rows = []
        for k in range(members):
            kb = k // SUB
            left = here[kb][k % SUB : k % SUB + 1]
            for jb in range(kb, blocks):
                right = here[jb]
                use = left
                if jb == kb and k % SUB == SUB - 1:
                    use = jnp.where(sub8 < SUB - 1, innov, left)
                if jb == kb and k % SUB == SUB - 2:
                    use = jnp.where(sub8 < 1, innov, left)
                    right = jnp.where(sub8 < 1, right[SUB - 1 : SUB], right)
                rows.append(use * right)
        for n in range(0, len(rows), 2):
            high, low = split(jnp.concatenate(rows[n : n + 2], axis=0))
            qhi[n * SUB : (n + 2) * SUB, at : at + O] = high
            qlo[n * SUB : (n + 2) * SUB, at : at + O] = low

    scale = -1.0 / (2.0 * LOC_SCALE * LOC_SCALE)
    middle = (HALF - 1) * 0.5
    t_id = lax.broadcasted_iota(jnp.int32, (SUB, O), 0)
    t_row = t_id >> 1
    t_mid = (t_id & 1).astype(f32) * HALF + middle
    col = lax.broadcasted_iota(jnp.int32, (T, O), 0)

    def row_weight(c, i):
        y = place[2 * i, c : c + 1, :]
        row_off = i + 1 - t_row
        dy = (row_off * SIDE).astype(f32) + y - t_mid
        return jnp.where(jnp.abs(row_off) <= 1, jnp.exp(dy * dy * scale), 0.0)

    def edge_weight(c, i, ly, away):
        x = place[2 * i + 1, c : c + 1, :]
        parts = []
        for pc in range(2):
            dx = away * SIDE + x - (pc * HALF + middle)
            parts.append(ly * jnp.exp(dx * dx * scale))
        return jnp.concatenate(parts, axis=0)

    def locality(c, i):
        at = (c * R + i) * O
        x = place[2 * i + 1, c : c + 1, :]
        ly = row_weight(c, i)
        col_off = c - col
        lx = []
        for pc in range(2):
            dx = (col_off * SIDE).astype(f32) + x - (pc * HALF + middle)
            lx.append(jnp.where(jnp.abs(col_off) <= 1, jnp.exp(dx * dx * scale), 0.0))

        def put(first, values):
            high, low = split(values)
            for at_row in first:
                lochi[at_row : at_row + values.shape[0], at : at + O] = high
                loclo[at_row : at_row + values.shape[0], at : at + O] = low

        for pc in range(2):
            for it in range(R):
                s = 2 * (it + 1)
                pair = jnp.concatenate([ly[s : s + 1] * lx[pc], ly[s + 1 : s + 2] * lx[pc]], axis=0)
                first = (pc * R + it) * 2 * T
                put((first, OWN // 2 + first), pair)
            for n, s in enumerate((0, 2 * (R + 1))):
                pair = jnp.concatenate([ly[s : s + 1] * lx[pc], ly[s + 1 : s + 2] * lx[pc]], axis=0)
                put((OWN + n * ROW_HALO + pc * 2 * T,), pair)
        if c == 0:
            put((used,), edge_weight(c, i, ly, 1))
        if c == T - 1:
            put((used + SIDE_HALO,), edge_weight(c, i, ly, -1))

    def dot(left, right):
        return lax.dot_general(left, right, NT, preferred_element_type=f32)

    def halo_plan(p, dm, dg):
        n = (dm + 1) * 3 + dg + 1
        send = row_ok[dg] if dg else jnp.bool_(True)
        recv = row_ok[-dg] if dg else jnp.bool_(True)
        at = p
        if dm == 0:
            first = 0 if dg < 0 else ROW_HALO
            src = halo_out.at[p, pl.ds(first, ROW_HALO)]
            dst = row_in.at[p, 0 if dg < 0 else 1]
            come = p
        else:
            if dm < 0:
                send = jnp.logical_and(send, jnp.logical_or(m > 0, p == 0))
                recv = jnp.logical_and(recv, jnp.logical_or(m < M - 1, p == 0))
            else:
                send = jnp.logical_and(send, jnp.logical_or(m < M - 1, p == 0))
                recv = jnp.logical_and(recv, jnp.logical_or(m > 0, p == 1))
                at = jnp.where(m == M - 1, 1, p)
            first = 2 * ROW_HALO + (0 if dm < 0 else SIDE_HALO)
            src = halo_out.at[p, pl.ds(first, SIDE_HALO)]
            base = (0 if dm < 0 else 3) + dg + 1
            dst = side_in.at[at, base]
            come = p

        def copy(slot, to_m, to_g):
            target = row_in.at[slot, 0 if dg < 0 else 1] if dm == 0 else side_in.at[slot, (0 if dm < 0 else 3) + dg + 1]
            return pltpu.make_async_remote_copy(
                src_ref=src, dst_ref=target, send_sem=halo_send.at[p, n], recv_sem=halo_recv.at[slot, n],
                device_id=(to_m, to_g), device_id_type=MESH,
            )

        outward = lambda: copy(at, lax.rem(m + M + dm, M), g + dg)
        inward = lambda: copy(p, lax.rem(m + M - dm, M), g - dg)
        landing = row_in.at[p, 0 if dg < 0 else 1] if dm == 0 else side_in.at[p, (0 if dm < 0 else 3) + dg + 1]
        return send, recv, outward, inward, landing

    near = [(dm, dg) for dm in (0, 1, -1) for dg in (-1, 0, 1) if (dm, dg) != (0, 0)]
    lane = lax.broadcasted_iota(jnp.int32, (SUB, OWN), 1)
    west = (lane & 32) == 0
    sub = lax.broadcasted_iota(jnp.int32, (SUB, OWN), 0)

    def square(left, right, into, first):
        for kb in range(blocks):
            for k0 in range(kb * SUB, (kb + 1) * SUB, 4):
                ks = range(k0, k0 + 4)
                sums = {}
                for i in range(members):
                    rights = [right[i * members + SUB * jb : i * members + SUB * (jb + 1), :] for jb in range(kb, blocks)]
                    for k in ks:
                        lone = left[k * members + i : k * members + i + 1, :]
                        for jb in range(kb, blocks):
                            term = lone * rights[jb - kb]
                            sums[k, jb] = term if i == 0 else sums[k, jb] + term
                for k in ks:
                    for jb in range(kb, blocks):
                        out = sums[k, jb]
                        if first:
                            out = -0.5 * out
                            if jb == kb:
                                out = out + jnp.where(sub == k % SUB, 1.5, 0.0)
                        put_entry(into, k, jb, out)

    def put_entry(into, k, jb, out):
        into[k * members + SUB * jb : k * members + SUB * (jb + 1), :] = out
        if jb > k // SUB:
            into[pl.ds(SUB * jb * members + k, SUB, stride=members), :] = out

    fields = V // CELLS
    halves = CELLS // LANES

    def phase(p, carry):
        first_phase = p == 0

        @pl.when(jnp.logical_or(first_phase, m > 0))
        def _():
            wait_ens(p)

        gather(p)
        for c in range(T):
            for i in range(R):
                products(c, i)
                locality(c, i)
        both = dot(qhi[...], lochi[...]) + dot(qhi[...], loclo[...]) + dot(qlo[...], lochi[...])
        own[...] = both[:, :OWN]
        halo_out[p] = jnp.transpose(both[:, OWN:])[: halo_out.shape[1]]

        plans = [halo_plan(p, dm, dg) for dm, dg in near]
        for (dm, dg), (send, recv, outward, inward, landing) in zip(near, plans):
            if dm >= 0:
                @pl.when(send)
                def _():
                    outward().start()

        @pl.when(jnp.logical_and(first_phase, m == 0))
        def _():
            wait_ens(1)
            gather(1)
            edges = []
            for i in range(R):
                products(0, i)
                edges.append(edge_weight(0, i, row_weight(0, i), 1))
            high, low = split(jnp.concatenate(edges, axis=1))
            seam = qhi[:, : R * O]
            halo_out[0, 2 * ROW_HALO : 2 * ROW_HALO + SIDE_HALO, :] = (
                dot(high, seam) + dot(low, seam) + dot(high, qlo[:, : R * O])
            )

        for (dm, dg), (send, recv, outward, inward, landing) in zip(near, plans):
            if dm < 0:
                @pl.when(send)
                def _():
                    outward().start()

        @pl.when(first_phase)
        def _():
            for off in order:
                to = lax.rem(m + off, M)
                @pl.when(to != 0)
                def _():
                    ens_copy(1, 1, off, to, m).start()

        total = None
        for k in range(members):
            rows = []
            for f in range(fields):
                part = [
                    ens[p, k, i, :, f * CELLS + h * LANES : f * CELLS + (h + 1) * LANES]
                    for i in range(R) for h in range(halves)
                ]
                rows += part + part
            turned = jnp.transpose(jnp.concatenate(rows, axis=0))
            lines = []
            for r in range(SUB):
                lines.append(jnp.where(west, turned[16 * r : 16 * r + 8], turned[16 * r + 8 : 16 * r + 16]))
            for r in range(SUB):
                xt[k, r * SUB : (r + 1) * SUB, :] = lines[r]
            total = lines if total is None else [a + b for a, b in zip(total, lines)]
        avg = [line * (1.0 / members) for line in total]
        for r in range(SUB):
            mean[r * SUB : (r + 1) * SUB, :] = avg[r]
        for k in range(members):
            for r in range(SUB):
                xt[k, r * SUB : (r + 1) * SUB, :] = xt[k, r * SUB : (r + 1) * SUB, :] - avg[r]

        for send, recv, outward, inward, landing in plans:
            @pl.when(recv)
            def _():
                inward().wait_recv()

            @pl.when(jnp.logical_not(recv))
            def _():
                landing[...] = jnp.zeros(landing.shape, f32)

        col8 = lax.broadcasted_iota(jnp.int32, (T, PACKED), 0)
        for pc in range(2):
            for i in range(R):
                for pr in range(2):
                    at = (pc * 2 + pr) * T
                    block = None
                    if i == R - 1:
                        block = row_in[p, 0, at : at + T, :]
                    if i == 0:
                        more = row_in[p, 1, at : at + T, :]
                        block = more if block is None else block + more
                    for base, at_col in ((0, T - 1), (3, 0)):
                        def pick(dg, t):
                            place_in = pc * SUB + t * 2 + pr
                            return side_in[p, base + dg + 1, place_in : place_in + 1, :]

                        line = pick(0, i + 1)
                        if i == R - 1:
                            line = line + pick(-1, 0)
                        if i == 0:
                            line = line + pick(1, R + 1)
                        more = jnp.where(col8 == at_col, line, 0.0)
                        block = more if block is None else block + more
                    at = ((pc * R + i) * 2 + pr) * T
                    hin[at : at + T, :] = block
                    hin[OWN // 2 + at : OWN // 2 + at + T, :] = block
        prec = own[...] + jnp.transpose(hin[...])

        for b in range(blocks):
            top = prec[row_of(SUB * b + SUB - 1, b) : row_of(SUB * b + SUB - 1, b) + SUB]
            last = prec[row_of(SUB * b + SUB - 2, b) : row_of(SUB * b + SUB - 2, b) + 1]
            drv[SUB * b : SUB * (b + 1), :] = jnp.where(sub < SUB - 1, top, last)
        y0, y1, z0, z1 = root.at[0], root.at[1], inv.at[0], inv.at[1]
        inflate = (members - 1) / INFLATION_FACTOR
        for k in range(members):
            kb = k // SUB
            for jb in range(kb, blocks):
                out = prec[row_of(k, jb) : row_of(k, jb) + SUB]
                if jb == kb:
                    keep = {SUB - 1: sub >= SUB - 1, SUB - 2: sub >= 1}.get(k % SUB)
                    if keep is not None:
                        out = jnp.where(keep, out, 0.0)
                    out = out + jnp.where(sub == k % SUB, inflate, 0.0)
                put_entry(y1, k, jb, out)
        for b in range(blocks):
            for e in (SUB - 1, SUB - 2):
                k = SUB * b + e
                y1[k * members + SUB * b : k * members + SUB * (b + 1), :] = y1[
                    pl.ds(SUB * b * members + k, SUB, stride=members), :
                ]
        squares = None
        for n in range(members * blocks):
            line = y1[n * SUB : (n + 1) * SUB, :]
            squares = line * line if squares is None else squares + line * line
        norm = jnp.sqrt(jnp.sum(squares, axis=0, keepdims=True))
        small = 1.0 / norm
        for k in range(members):
            for jb in range(blocks):
                rows = slice(k * members + SUB * jb, k * members + SUB * (jb + 1))
                start = y1[rows, :] * small
                first_m = -0.5 * start
                if jb == k // SUB:
                    first_m = first_m + jnp.where(sub == k % SUB, 1.5, 0.0)
                y1[rows, :] = start
                step[rows, :] = first_m
                z0[rows, :] = first_m
        square(y1, step, y0, False)

        def sweep(n, carry):
            now = lax.rem(n, 2)
            square(inv.at[now], root.at[now], step, True)
            square(root.at[now], step, root.at[1 - now], False)
            square(inv.at[now], step, inv.at[1 - now], False)
            return carry

        lax.fori_loop(0, NS_ITERS - 2, sweep, 0)
        square(z0, y0, step, True)
        square(z0, step, z1, False)

        shrink = 1.0 / jnp.sqrt(norm)

        def applied(vector):
            sums = [None] * blocks
            for i in range(members):
                lone = vector[i : i + 1, :]
                for jb in range(blocks):
                    term = lone * z1[i * members + SUB * jb : i * members + SUB * (jb + 1), :]
                    sums[jb] = term if i == 0 else sums[jb] + term
            return [line * shrink for line in sums]

        for jb, line in enumerate(applied(drv)):
            half_ref[SUB * jb : SUB * (jb + 1), :] = line
        mean_w = applied(half_ref)
        spread = math.sqrt(members - 1) * shrink
        for k in range(members):
            for jb in range(blocks):
                wt[k, SUB * jb : SUB * (jb + 1), :] = (
                    mean_w[jb] + spread * z1[k * members + SUB * jb : k * members + SUB * (jb + 1), :]
                )

        chips = M // 2
        group = 2 * K

        def update(q, carry):
            away_chip = jnp.where(q == 0, chips // 2, jnp.where(q == chips - 1, 0, jnp.where(q == 1, 1, chips - 1)))
            chip = lax.rem(m // 2 + away_chip, chips)
            k0 = chip * group
            for pair in range(0, group, 2):
                sums = [[mean[r * SUB : (r + 1) * SUB, :] for r in range(SUB)] for _ in range(2)]
                for j in range(members):
                    lines = [xt[j, r * SUB : (r + 1) * SUB, :] for r in range(SUB)]
                    for e in range(2):
                        lone = wt[k0 + pair + e, j : j + 1, :]
                        sums[e] = [s + lone * line for s, line in zip(sums[e], lines)]
                rows = []
                for r in range(SUB):
                    one, two = sums[0][r], sums[1][r]
                    rows.append(jnp.where(west, one, pltpu.roll(two, 32, 1)))
                    rows.append(jnp.where(west, pltpu.roll(one, OWN - 32, 1), two))
                turned = jnp.transpose(jnp.concatenate(rows, axis=0))
                at = 0
                for f in range(fields):
                    for e in range(2):
                        for i in range(R):
                            for h in range(halves):
                                lanes = f * CELLS + h * LANES
                                outgoing[p, k0 + pair + e, i, :, lanes : lanes + LANES] = turned[at : at + T]
                                at += T
            for core in range(2):
                dest = 2 * chip + core
                away = lax.rem(dest - m + M, M)

                @pl.when(away != 0)
                def _():
                    out_copy(p, away, dest, m).start()

                @pl.when(away == 0)
                def _():
                    out_ref[:, :, tile(p, m), :] = outgoing[p, pl.ds(dest * K, K)]
            return carry

        lax.fori_loop(0, chips, update, 0)
        return carry

    def out_copy(p, away, dest, source):
        return pltpu.make_async_remote_copy(
            src_ref=outgoing.at[p, pl.ds(dest * K, K)],
            dst_ref=out_ref.at[:, :, tile(p, source), :],
            send_sem=out_send.at[p, away], recv_sem=out_recv.at[p, away],
            device_id=(dest, g), device_id_type=MESH,
        )

    lax.fori_loop(0, PHASES, phase, 0)

    for off in range(1, G):
        to = lax.rem(g + off, G)
        obs_copy(col_owner, to, to, col_phase, col_at).wait_send()

    @pl.when(col_owner != m)
    def _():
        obs_copy(col_owner, g, g, col_phase, col_at).wait_send()

    for p in range(PHASES):
        for n in range(2):
            for off in range(1, M):
                ens_copy(p, n, off, lax.rem(m + off, M), m).wait_send()
        for dm, dg in near:
            send, recv, outward, inward, landing = halo_plan(p, dm, dg)

            @pl.when(send)
            def _():
                outward().wait_send()
    for p in range(PHASES):
        for off in range(1, M):
            out_copy(p, off, lax.rem(m + off, M), m).wait_send()
            out_copy(p, off, m, lax.rem(m + M - off, M)).wait_recv()


def local(M, G, ensemble, obs_value, obs_error, obs_index, obs_count):
    K, R, cols, V = ensemble.shape
    O = obs_value.shape[2]
    members = M * K
    assert cols == PHASES * M * T and cols == M * G and R == 2 and members == 24 and V == 2 * CELLS and O == LANES
    wide = T * R * O
    packed = 384
    square = members * members
    f32 = jnp.float32
    vmem = pltpu.VMEM
    dma = pltpu.SemaphoreType.DMA
    flat = lambda a: a.reshape(a.shape[0], -1)
    return pl.pallas_call(
        functools.partial(kernel, (M, G, K, R, V, O)),
        out_shape=pltpu.VMEM(ensemble.shape, f32),
        in_specs=[pl.BlockSpec(memory_space=pl.ANY)] * 4
        + [pl.BlockSpec(memory_space=pltpu.SMEM)],
        out_specs=pl.BlockSpec(memory_space=vmem),
        scratch_shapes=[
            vmem((G * R, O), f32),
            vmem((G * R, O), f32),
            vmem((G * R, O), jnp.int32),
            vmem((PHASES, members, R, T, V), f32),
            vmem((G * SUB, O), f32),
            vmem((PHASES, T * SUB, O), f32),
            vmem((R, (members + 1) * T, O), f32),
            vmem((2 * R, T, O), f32),
            vmem((TARGETS, wide), jnp.bfloat16),
            vmem((TARGETS, wide), jnp.bfloat16),
            vmem((packed, wide), jnp.bfloat16),
            vmem((packed, wide), jnp.bfloat16),
            vmem((packed, OWN), f32),
            vmem((OWN, packed), f32),
            vmem((PHASES, 2 * ROW_HALO + 2 * SIDE_HALO, packed), f32),
            vmem((PHASES, 2, ROW_HALO, packed), f32),
            vmem((PHASES, 6, SIDE_HALO, packed), f32),
            vmem((2, square, OWN), f32),
            vmem((2, square, OWN), f32),
            vmem((square, OWN), f32),
            vmem((members, OWN), f32),
            vmem((members, OWN), f32),
            vmem((members, members, OWN), f32),
            vmem((members, SUB * SUB, OWN), f32),
            vmem((SUB * SUB, OWN), f32),
            vmem((PHASES, members, R, T, V), f32),
            dma((PHASES, 2, M)), dma((PHASES, 2, M)), dma((G,)), dma((PHASES, T)),
            dma((PHASES, 9)), dma((PHASES, 9)), dma((PHASES, M)), dma((PHASES, M)), dma((3,)), dma((PHASES,)),
        ],
        compiler_params=pltpu.CompilerParams(
            collective_id=0, has_side_effects=True, vmem_limit_bytes=56 * 1024 * 1024
        ),
    )(ensemble, flat(obs_value), flat(obs_error), flat(obs_index), obs_count.reshape(1, -1))


def solution(mesh):
    return jax.shard_map(
        functools.partial(local, mesh.shape["member"], mesh.shape["region"]),
        mesh=mesh,
        in_specs=(
            P("member", "region", None, None),
            P(None, ("member", "region"), None),
            P(None, ("member", "region"), None),
            P(None, ("member", "region"), None),
            P(None, ("member", "region")),
        ),
        out_specs=P("member", "region", None, None),
        check_vma=False,
    )
```

```python
import functools
import math

import jax
import jax.numpy as jnp
from jax import lax
from jax.experimental import pallas as pl
from jax.experimental.pallas import tpu as pltpu
from jax.sharding import PartitionSpec as P

SIDE = 16
CELLS = SIDE * SIDE
HALF = SIDE // 2
LANES = 128
SUB = 8
NS_ITERS = 6
LOC_SCALE = 12.0
INFLATION_FACTOR = 1.1
MESH = pl.DeviceIdType.MESH
NT = (((1,), (1,)), ((), ()))
T = 8
PHASES = 2
OWN = 128
ROW_HALO = 32
SIDE_HALO = 16
TARGETS = 256


def split(values):
    high = values.astype(jnp.bfloat16)
    low = (values - high.astype(jnp.float32)).astype(jnp.bfloat16)
    return high, low


def row_of(k, jb):
    kb = k // SUB
    return (0, 192, 320)[kb] + (k - SUB * kb) * (24 - SUB * kb) + SUB * (jb - kb)


def kernel(
    dims,
    ens_ref, value_any, error_any, index_any, count_ref, out_ref,
    value_ref, error_ref, index_ref, ens, pack, obs, slots, place, lochi, loclo, qhi, qlo, own, hin,
    halo_out, row_in, side_in, root, inv, step, drv, half_ref, wt, xt, mean, outgoing,
    ens_send, ens_recv, obs_send, obs_recv, halo_send, halo_recv, out_send, out_recv, local_sem, own_sem, entry_sem,
):
    M, G, K, R, V, O = dims
    members = M * K
    blocks = members // SUB
    PACKED = own.shape[0]
    m = lax.axis_index("member")
    g = lax.axis_index("region")
    f32 = jnp.float32

    loads = []
    for n, (src, dst) in enumerate(((value_any, value_ref), (error_any, error_ref), (index_any, index_ref))):
        load = pltpu.make_async_copy(src, dst, local_sem.at[n])
        load.start()
        loads.append(load)

    def tile(p, d):
        return pl.ds(pl.multiple_of((p * M + d) * T, T), T)

    def own_copy(p):
        return pltpu.make_async_copy(
            ens_ref.at[:, :, tile(p, m), :], ens.at[p, pl.ds(m * K, K)], own_sem.at[p]
        )

    for p in range(PHASES):
        own_copy(p).start()

    column = m * G + g
    col_tile = column // T
    col_owner = lax.rem(col_tile, M)
    col_phase = col_tile // M
    col_at = lax.rem(column, T)
    holders = []
    for s in range(PHASES * T):
        c = ((s // T) * M + m) * T + s % T
        holders.append((c // G, lax.rem(c, G)))

    ring = 4
    y, z = lax.rem(g, ring), g // ring
    x_peers = [(lax.rem(m + off, M), g) for off in range(1, M)]
    y_peers = [(m, z * ring + lax.rem(y + off, ring)) for off in range(1, ring)]
    z_peers = [(m, lax.rem(g + off * ring, G)) for off in range(1, G // ring)]
    barrier = pltpu.get_barrier_semaphore()
    for peer in x_peers + y_peers + z_peers:
        pl.semaphore_signal(barrier, inc=1, device_id=peer, device_id_type=MESH)
    up_ok = g > 0
    down_ok = g < G - 1
    row_ok = {-1: up_ok, 1: down_ok}
    pl.semaphore_wait(barrier, len(x_peers) + len(y_peers) + len(z_peers))
    for peer in y_peers:
        pl.semaphore_signal(entry_sem.at[0], inc=1, device_id=peer, device_id_type=MESH)

    pieces = ((0, 1), (1, K))

    def ens_copy(p, n, off, to, at):
        a, b = pieces[n]
        return pltpu.make_async_remote_copy(
            src_ref=ens_ref.at[a:b, :, tile(p, to), :],
            dst_ref=ens.at[p, pl.ds(at * K + a, b - a)],
            send_sem=ens_send.at[p, n, off], recv_sem=ens_recv.at[p, n, off],
            device_id=(to, g), device_id_type=MESH,
        )

    order = [4, 5, 3, 2, 6, 1, 7]
    order = [off for off in order if off < M] + [off for off in range(1, M) if off not in order]
    for n in range(2):
        for off in order:
            ens_copy(0, n, off, lax.rem(m + off, M), m).start()
    pl.semaphore_wait(entry_sem.at[0], len(y_peers))
    for peer in x_peers:
        pl.semaphore_signal(entry_sem.at[1], inc=1, device_id=peer, device_id_type=MESH)
    for off in order:
        ens_copy(1, 0, off, lax.rem(m + off, M), m).start()
    for off in order:
        to = lax.rem(m + off, M)
        @pl.when(to == 0)
        def _():
            ens_copy(1, 1, off, to, m).start()

    for load in loads:
        load.wait()
    slot = lax.broadcasted_iota(jnp.int32, (G * R, O), 1)
    slot_row = lax.broadcasted_iota(jnp.int32, (G * R, O), 0)
    count = jnp.zeros((G * R, O), jnp.int32)
    for d in range(G * R):
        count = jnp.where(slot_row == d, count_ref[0, d], count)
    live = jnp.where(slot < count, 1.0, 0.0).astype(f32)
    weight = jnp.sqrt(live / error_ref[...])
    value = value_ref[...]
    index_f = index_ref[...].astype(f32)
    for d in range(G):
        base = d * SUB
        pack[base : base + R, :] = weight[d * R : (d + 1) * R]
        pack[base + R : base + 2 * R, :] = value[d * R : (d + 1) * R]
        pack[base + 2 * R : base + 3 * R, :] = index_f[d * R : (d + 1) * R]
        pack[base + 3 * R : base + SUB, :] = jnp.zeros((SUB - 3 * R, O), f32)
    used = OWN + 2 * ROW_HALO
    lochi[used:, :] = jnp.zeros((TARGETS - used, lochi.shape[1]), jnp.bfloat16)
    loclo[used:, :] = jnp.zeros((TARGETS - used, lochi.shape[1]), jnp.bfloat16)

    pl.semaphore_wait(entry_sem.at[1], len(x_peers))

    def obs_copy(to_m, to_g, src_g, p, e):
        return pltpu.make_async_remote_copy(
            src_ref=pack.at[pl.ds(pl.multiple_of(src_g * SUB, SUB), SUB)],
            dst_ref=obs.at[p, pl.ds(pl.multiple_of(e * SUB, SUB), SUB)],
            send_sem=obs_send.at[src_g], recv_sem=obs_recv.at[p, e],
            device_id=(to_m, to_g), device_id_type=MESH,
        )

    for off in range(1, G):
        to = lax.rem(g + off, G)
        obs_copy(col_owner, to, to, col_phase, col_at).start()

    @pl.when(col_owner != m)
    def _():
        obs_copy(col_owner, g, g, col_phase, col_at).start()

    @pl.when(col_owner == m)
    def _():
        obs[col_phase, pl.ds(pl.multiple_of(col_at * SUB, SUB), SUB), :] = pack[
            pl.ds(pl.multiple_of(g * SUB, SUB), SUB), :
        ]

    for s, (hm, hg) in enumerate(holders):
        @pl.when(jnp.logical_not(jnp.logical_and(hm == m, hg == g)))
        def _():
            obs_copy(hm, hg, g, s // T, s % T).wait_recv()

    def wait_ens(p):
        own_copy(p).wait()
        for n in range(2):
            for off in range(1, M):
                came = lax.rem(m + M - off, M)
                ens_copy(p, n, off, came, came).wait_recv()

    tiles = V // LANES

    def gather(p):
        for i in range(R):
            wgt = obs[p, pl.ds(i, T, stride=SUB), :]
            val = obs[p, pl.ds(R + i, T, stride=SUB), :]
            idx = obs[p, pl.ds(2 * R + i, T, stride=SUB), :].astype(jnp.int32)
            lane = idx & (LANES - 1)
            which = idx >> 7
            cell = idx & (CELLS - 1)
            place[2 * i] = (cell >> 4).astype(f32)
            place[2 * i + 1] = (cell & (SIDE - 1)).astype(f32)
            seen = []
            for k in range(members):
                got = jnp.take_along_axis(ens[p, k, i, :, :LANES], lane, axis=1)
                for t in range(1, tiles):
                    more = jnp.take_along_axis(ens[p, k, i, :, t * LANES : (t + 1) * LANES], lane, axis=1)
                    got = jnp.where(which == t, more, got)
                seen.append(got)
            total = seen[0]
            for k in range(1, members):
                total = total + seen[k]
            avg = total * (1.0 / members)
            for k in range(members):
                slots[i, k * T : (k + 1) * T, :] = wgt * (seen[k] - avg)
            slots[i, members * T : (members + 1) * T, :] = wgt * (val - avg)

    sub8 = lax.broadcasted_iota(jnp.int32, (SUB, O), 0)

    def products(c, i):
        at = (c * R + i) * O
        here = [slots[i, pl.ds(c + b * SUB * T, SUB, stride=T), :] for b in range(blocks)]
        innov = slots[i, members * T + c : members * T + c + 1, :]
        rows = []
        for k in range(members):
            kb = k // SUB
            left = here[kb][k % SUB : k % SUB + 1]
            for jb in range(kb, blocks):
                right = here[jb]
                use = left
                if jb == kb and k % SUB == SUB - 1:
                    use = jnp.where(sub8 < SUB - 1, innov, left)
                if jb == kb and k % SUB == SUB - 2:
                    use = jnp.where(sub8 < 1, innov, left)
                    right = jnp.where(sub8 < 1, right[SUB - 1 : SUB], right)
                rows.append(use * right)
        for n in range(0, len(rows), 2):
            high, low = split(jnp.concatenate(rows[n : n + 2], axis=0))
            qhi[n * SUB : (n + 2) * SUB, at : at + O] = high
            qlo[n * SUB : (n + 2) * SUB, at : at + O] = low

    scale = -1.0 / (2.0 * LOC_SCALE * LOC_SCALE)
    middle = (HALF - 1) * 0.5
    t_id = lax.broadcasted_iota(jnp.int32, (SUB, O), 0)
    t_row = t_id >> 1
    t_mid = (t_id & 1).astype(f32) * HALF + middle
    col = lax.broadcasted_iota(jnp.int32, (T, O), 0)

    def row_weight(c, i):
        y = place[2 * i, c : c + 1, :]
        row_off = i + 1 - t_row
        dy = (row_off * SIDE).astype(f32) + y - t_mid
        return jnp.where(jnp.abs(row_off) <= 1, jnp.exp(dy * dy * scale), 0.0)

    def edge_weight(c, i, ly, away):
        x = place[2 * i + 1, c : c + 1, :]
        parts = []
        for pc in range(2):
            dx = away * SIDE + x - (pc * HALF + middle)
            parts.append(ly * jnp.exp(dx * dx * scale))
        return jnp.concatenate(parts, axis=0)

    def locality(c, i):
        at = (c * R + i) * O
        x = place[2 * i + 1, c : c + 1, :]
        ly = row_weight(c, i)
        col_off = c - col
        lx = []
        for pc in range(2):
            dx = (col_off * SIDE).astype(f32) + x - (pc * HALF + middle)
            lx.append(jnp.where(jnp.abs(col_off) <= 1, jnp.exp(dx * dx * scale), 0.0))

        def put(first, values):
            high, low = split(values)
            for at_row in first:
                lochi[at_row : at_row + values.shape[0], at : at + O] = high
                loclo[at_row : at_row + values.shape[0], at : at + O] = low

        for pc in range(2):
            for it in range(R):
                s = 2 * (it + 1)
                pair = jnp.concatenate([ly[s : s + 1] * lx[pc], ly[s + 1 : s + 2] * lx[pc]], axis=0)
                first = (pc * R + it) * 2 * T
                put((first, OWN // 2 + first), pair)
            for n, s in enumerate((0, 2 * (R + 1))):
                pair = jnp.concatenate([ly[s : s + 1] * lx[pc], ly[s + 1 : s + 2] * lx[pc]], axis=0)
                put((OWN + n * ROW_HALO + pc * 2 * T,), pair)
        if c == 0:
            put((used,), edge_weight(c, i, ly, 1))
        if c == T - 1:
            put((used + SIDE_HALO,), edge_weight(c, i, ly, -1))

    def dot(left, right):
        return lax.dot_general(left, right, NT, preferred_element_type=f32)

    def halo_plan(p, dm, dg):
        n = (dm + 1) * 3 + dg + 1
        send = row_ok[dg] if dg else jnp.bool_(True)
        recv = row_ok[-dg] if dg else jnp.bool_(True)
        at = p
        if dm == 0:
            first = 0 if dg < 0 else ROW_HALO
            src = halo_out.at[p, pl.ds(first, ROW_HALO)]
            dst = row_in.at[p, 0 if dg < 0 else 1]
            come = p
        else:
            if dm < 0:
                send = jnp.logical_and(send, jnp.logical_or(m > 0, p == 0))
                recv = jnp.logical_and(recv, jnp.logical_or(m < M - 1, p == 0))
            else:
                send = jnp.logical_and(send, jnp.logical_or(m < M - 1, p == 0))
                recv = jnp.logical_and(recv, jnp.logical_or(m > 0, p == 1))
                at = jnp.where(m == M - 1, 1, p)
            first = 2 * ROW_HALO + (0 if dm < 0 else SIDE_HALO)
            src = halo_out.at[p, pl.ds(first, SIDE_HALO)]
            base = (0 if dm < 0 else 3) + dg + 1
            dst = side_in.at[at, base]
            come = p

        def copy(slot, to_m, to_g):
            target = row_in.at[slot, 0 if dg < 0 else 1] if dm == 0 else side_in.at[slot, (0 if dm < 0 else 3) + dg + 1]
            return pltpu.make_async_remote_copy(
                src_ref=src, dst_ref=target, send_sem=halo_send.at[p, n], recv_sem=halo_recv.at[slot, n],
                device_id=(to_m, to_g), device_id_type=MESH,
            )

        outward = lambda: copy(at, lax.rem(m + M + dm, M), g + dg)
        inward = lambda: copy(p, lax.rem(m + M - dm, M), g - dg)
        landing = row_in.at[p, 0 if dg < 0 else 1] if dm == 0 else side_in.at[p, (0 if dm < 0 else 3) + dg + 1]
        return send, recv, outward, inward, landing

    near = [(dm, dg) for dm in (0, 1, -1) for dg in (-1, 0, 1) if (dm, dg) != (0, 0)]
    lane = lax.broadcasted_iota(jnp.int32, (SUB, OWN), 1)
    west = (lane & 32) == 0
    sub = lax.broadcasted_iota(jnp.int32, (SUB, OWN), 0)

    def square(left, right, into, first):
        for kb in range(blocks):
            for k0 in range(kb * SUB, (kb + 1) * SUB, 4):
                ks = range(k0, k0 + 4)
                sums = {}
                for i in range(members):
                    rights = [right[i * members + SUB * jb : i * members + SUB * (jb + 1), :] for jb in range(kb, blocks)]
                    for k in ks:
                        lone = left[k * members + i : k * members + i + 1, :]
                        for jb in range(kb, blocks):
                            term = lone * rights[jb - kb]
                            sums[k, jb] = term if i == 0 else sums[k, jb] + term
                for k in ks:
                    for jb in range(kb, blocks):
                        out = sums[k, jb]
                        if first:
                            out = -0.5 * out
                            if jb == kb:
                                out = out + jnp.where(sub == k % SUB, 1.5, 0.0)
                        put_entry(into, k, jb, out)

    def put_entry(into, k, jb, out):
        into[k * members + SUB * jb : k * members + SUB * (jb + 1), :] = out
        if jb > k // SUB:
            into[pl.ds(SUB * jb * members + k, SUB, stride=members), :] = out

    fields = V // CELLS
    halves = CELLS // LANES

    def results(p):
        chips = M // 2
        group = 2 * K

        def update(q, carry):
            away_chip = jnp.where(q == 0, chips // 2, jnp.where(q == chips - 1, 0, jnp.where(q == 1, 1, chips - 1)))
            chip = lax.rem(m // 2 + away_chip, chips)
            k0 = chip * group
            for pair in range(0, group, 2):
                sums = [[mean[r * SUB : (r + 1) * SUB, :] for r in range(SUB)] for _ in range(2)]
                for j in range(members):
                    lines = [xt[j, r * SUB : (r + 1) * SUB, :] for r in range(SUB)]
                    for e in range(2):
                        lone = wt[k0 + pair + e, j : j + 1, :]
                        sums[e] = [s + lone * line for s, line in zip(sums[e], lines)]
                rows = []
                for r in range(SUB):
                    one, two = sums[0][r], sums[1][r]
                    rows.append(jnp.where(west, one, pltpu.roll(two, 32, 1)))
                    rows.append(jnp.where(west, pltpu.roll(one, OWN - 32, 1), two))
                turned = jnp.transpose(jnp.concatenate(rows, axis=0))
                at = 0
                for f in range(fields):
                    for e in range(2):
                        for i in range(R):
                            for h in range(halves):
                                lanes = f * CELLS + h * LANES
                                outgoing[p, k0 + pair + e, i, :, lanes : lanes + LANES] = turned[at : at + T]
                                at += T
            for core in range(2):
                dest = 2 * chip + core
                away = lax.rem(dest - m + M, M)

                @pl.when(away != 0)
                def _():
                    out_copy(p, away, dest, m).start()

                @pl.when(away == 0)
                def _():
                    out_ref[:, :, tile(p, m), :] = outgoing[p, pl.ds(dest * K, K)]
            return carry

        lax.fori_loop(0, chips, update, 0)

    def phase(p, carry):
        first_phase = p == 0

        @pl.when(jnp.logical_or(first_phase, m > 0))
        def _():
            wait_ens(p)

        gather(p)
        for c in range(T):
            for i in range(R):
                products(c, i)
                locality(c, i)
        both = dot(qhi[...], lochi[...]) + dot(qhi[...], loclo[...]) + dot(qlo[...], lochi[...])
        own[...] = both[:, :OWN]
        halo_out[p] = jnp.transpose(both[:, OWN:])[: halo_out.shape[1]]

        plans = [halo_plan(p, dm, dg) for dm, dg in near]
        for (dm, dg), (send, recv, outward, inward, landing) in zip(near, plans):
            if dm >= 0:
                @pl.when(send)
                def _():
                    outward().start()

        @pl.when(jnp.logical_and(first_phase, m == 0))
        def _():
            wait_ens(1)
            gather(1)
            edges = []
            for i in range(R):
                products(0, i)
                edges.append(edge_weight(0, i, row_weight(0, i), 1))
            high, low = split(jnp.concatenate(edges, axis=1))
            seam = qhi[:, : R * O]
            halo_out[0, 2 * ROW_HALO : 2 * ROW_HALO + SIDE_HALO, :] = (
                dot(high, seam) + dot(low, seam) + dot(high, qlo[:, : R * O])
            )

        for (dm, dg), (send, recv, outward, inward, landing) in zip(near, plans):
            if dm < 0:
                @pl.when(send)
                def _():
                    outward().start()

        @pl.when(first_phase)
        def _():
            for off in order:
                to = lax.rem(m + off, M)
                @pl.when(to != 0)
                def _():
                    ens_copy(1, 1, off, to, m).start()

        @pl.when(p > 0)
        def _():
            results(p - 1)

        total = None
        for k in range(members):
            rows = []
            for f in range(fields):
                part = [
                    ens[p, k, i, :, f * CELLS + h * LANES : f * CELLS + (h + 1) * LANES]
                    for i in range(R) for h in range(halves)
                ]
                rows += part + part
            turned = jnp.transpose(jnp.concatenate(rows, axis=0))
            lines = []
            for r in range(SUB):
                lines.append(jnp.where(west, turned[16 * r : 16 * r + 8], turned[16 * r + 8 : 16 * r + 16]))
            for r in range(SUB):
                xt[k, r * SUB : (r + 1) * SUB, :] = lines[r]
            total = lines if total is None else [a + b for a, b in zip(total, lines)]
        avg = [line * (1.0 / members) for line in total]
        for r in range(SUB):
            mean[r * SUB : (r + 1) * SUB, :] = avg[r]
        for k in range(members):
            for r in range(SUB):
                xt[k, r * SUB : (r + 1) * SUB, :] = xt[k, r * SUB : (r + 1) * SUB, :] - avg[r]

        for send, recv, outward, inward, landing in plans:
            @pl.when(recv)
            def _():
                inward().wait_recv()

            @pl.when(jnp.logical_not(recv))
            def _():
                landing[...] = jnp.zeros(landing.shape, f32)

        col8 = lax.broadcasted_iota(jnp.int32, (T, PACKED), 0)
        for pc in range(2):
            for i in range(R):
                for pr in range(2):
                    at = (pc * 2 + pr) * T
                    block = None
                    if i == R - 1:
                        block = row_in[p, 0, at : at + T, :]
                    if i == 0:
                        more = row_in[p, 1, at : at + T, :]
                        block = more if block is None else block + more
                    for base, at_col in ((0, T - 1), (3, 0)):
                        def pick(dg, t):
                            place_in = pc * SUB + t * 2 + pr
                            return side_in[p, base + dg + 1, place_in : place_in + 1, :]

                        line = pick(0, i + 1)
                        if i == R - 1:
                            line = line + pick(-1, 0)
                        if i == 0:
                            line = line + pick(1, R + 1)
                        more = jnp.where(col8 == at_col, line, 0.0)
                        block = more if block is None else block + more
                    at = ((pc * R + i) * 2 + pr) * T
                    hin[at : at + T, :] = block
                    hin[OWN // 2 + at : OWN // 2 + at + T, :] = block
        prec = own[...] + jnp.transpose(hin[...])

        for b in range(blocks):
            top = prec[row_of(SUB * b + SUB - 1, b) : row_of(SUB * b + SUB - 1, b) + SUB]
            last = prec[row_of(SUB * b + SUB - 2, b) : row_of(SUB * b + SUB - 2, b) + 1]
            drv[SUB * b : SUB * (b + 1), :] = jnp.where(sub < SUB - 1, top, last)
        y0, y1, z0, z1 = root.at[0], root.at[1], inv.at[0], inv.at[1]
        inflate = (members - 1) / INFLATION_FACTOR
        for k in range(members):
            kb = k // SUB
            for jb in range(kb, blocks):
                out = prec[row_of(k, jb) : row_of(k, jb) + SUB]
                if jb == kb:
                    keep = {SUB - 1: sub >= SUB - 1, SUB - 2: sub >= 1}.get(k % SUB)
                    if keep is not None:
                        out = jnp.where(keep, out, 0.0)
                    out = out + jnp.where(sub == k % SUB, inflate, 0.0)
                put_entry(y1, k, jb, out)
        for b in range(blocks):
            for e in (SUB - 1, SUB - 2):
                k = SUB * b + e
                y1[k * members + SUB * b : k * members + SUB * (b + 1), :] = y1[
                    pl.ds(SUB * b * members + k, SUB, stride=members), :
                ]
        squares = None
        for n in range(members * blocks):
            line = y1[n * SUB : (n + 1) * SUB, :]
            squares = line * line if squares is None else squares + line * line
        norm = jnp.sqrt(jnp.sum(squares, axis=0, keepdims=True))
        small = 1.0 / norm
        for k in range(members):
            for jb in range(blocks):
                rows = slice(k * members + SUB * jb, k * members + SUB * (jb + 1))
                start = y1[rows, :] * small
                first_m = -0.5 * start
                if jb == k // SUB:
                    first_m = first_m + jnp.where(sub == k % SUB, 1.5, 0.0)
                y1[rows, :] = start
                step[rows, :] = first_m
                z0[rows, :] = first_m
        square(y1, step, y0, False)

        def sweep(n, carry):
            now = lax.rem(n, 2)
            square(inv.at[now], root.at[now], step, True)
            square(root.at[now], step, root.at[1 - now], False)
            square(inv.at[now], step, inv.at[1 - now], False)
            return carry

        lax.fori_loop(0, NS_ITERS - 2, sweep, 0)
        square(z0, y0, step, True)
        square(z0, step, z1, False)

        shrink = 1.0 / jnp.sqrt(norm)

        def applied(vector):
            sums = [None] * blocks
            for i in range(members):
                lone = vector[i : i + 1, :]
                for jb in range(blocks):
                    term = lone * z1[i * members + SUB * jb : i * members + SUB * (jb + 1), :]
                    sums[jb] = term if i == 0 else sums[jb] + term
            return [line * shrink for line in sums]

        for jb, line in enumerate(applied(drv)):
            half_ref[SUB * jb : SUB * (jb + 1), :] = line
        mean_w = applied(half_ref)
        spread = math.sqrt(members - 1) * shrink
        for k in range(members):
            for jb in range(blocks):
                wt[k, SUB * jb : SUB * (jb + 1), :] = (
                    mean_w[jb] + spread * z1[k * members + SUB * jb : k * members + SUB * (jb + 1), :]
                )

        return carry

    def out_copy(p, away, dest, source):
        return pltpu.make_async_remote_copy(
            src_ref=outgoing.at[p, pl.ds(dest * K, K)],
            dst_ref=out_ref.at[:, :, tile(p, source), :],
            send_sem=out_send.at[p, away], recv_sem=out_recv.at[p, away],
            device_id=(dest, g), device_id_type=MESH,
        )

    lax.fori_loop(0, PHASES, phase, 0)
    results(PHASES - 1)

    for off in range(1, G):
        to = lax.rem(g + off, G)
        obs_copy(col_owner, to, to, col_phase, col_at).wait_send()

    @pl.when(col_owner != m)
    def _():
        obs_copy(col_owner, g, g, col_phase, col_at).wait_send()

    for p in range(PHASES):
        for n in range(2):
            for off in range(1, M):
                ens_copy(p, n, off, lax.rem(m + off, M), m).wait_send()
        for dm, dg in near:
            send, recv, outward, inward, landing = halo_plan(p, dm, dg)

            @pl.when(send)
            def _():
                outward().wait_send()
    for p in range(PHASES):
        for off in range(1, M):
            out_copy(p, off, lax.rem(m + off, M), m).wait_send()
            out_copy(p, off, m, lax.rem(m + M - off, M)).wait_recv()


def local(M, G, ensemble, obs_value, obs_error, obs_index, obs_count):
    K, R, cols, V = ensemble.shape
    O = obs_value.shape[2]
    members = M * K
    assert cols == PHASES * M * T and cols == M * G and R == 2 and members == 24 and V == 2 * CELLS and O == LANES
    wide = T * R * O
    packed = 384
    square = members * members
    f32 = jnp.float32
    vmem = pltpu.VMEM
    dma = pltpu.SemaphoreType.DMA
    flat = lambda a: a.reshape(a.shape[0], -1)
    return pl.pallas_call(
        functools.partial(kernel, (M, G, K, R, V, O)),
        out_shape=pltpu.VMEM(ensemble.shape, f32),
        in_specs=[pl.BlockSpec(memory_space=pl.ANY)] * 4
        + [pl.BlockSpec(memory_space=pltpu.SMEM)],
        out_specs=pl.BlockSpec(memory_space=vmem),
        scratch_shapes=[
            vmem((G * R, O), f32),
            vmem((G * R, O), f32),
            vmem((G * R, O), jnp.int32),
            vmem((PHASES, members, R, T, V), f32),
            vmem((G * SUB, O), f32),
            vmem((PHASES, T * SUB, O), f32),
            vmem((R, (members + 1) * T, O), f32),
            vmem((2 * R, T, O), f32),
            vmem((TARGETS, wide), jnp.bfloat16),
            vmem((TARGETS, wide), jnp.bfloat16),
            vmem((packed, wide), jnp.bfloat16),
            vmem((packed, wide), jnp.bfloat16),
            vmem((packed, OWN), f32),
            vmem((OWN, packed), f32),
            vmem((PHASES, 2 * ROW_HALO + 2 * SIDE_HALO, packed), f32),
            vmem((PHASES, 2, ROW_HALO, packed), f32),
            vmem((PHASES, 6, SIDE_HALO, packed), f32),
            vmem((2, square, OWN), f32),
            vmem((2, square, OWN), f32),
            vmem((square, OWN), f32),
            vmem((members, OWN), f32),
            vmem((members, OWN), f32),
            vmem((members, members, OWN), f32),
            vmem((members, SUB * SUB, OWN), f32),
            vmem((SUB * SUB, OWN), f32),
            vmem((PHASES, members, R, T, V), f32),
            dma((PHASES, 2, M)), dma((PHASES, 2, M)), dma((G,)), dma((PHASES, T)),
            dma((PHASES, 9)), dma((PHASES, 9)), dma((PHASES, M)), dma((PHASES, M)), dma((3,)), dma((PHASES,)),
            pltpu.SemaphoreType.REGULAR((2,)),
        ],
        compiler_params=pltpu.CompilerParams(
            collective_id=0, has_side_effects=True, vmem_limit_bytes=56 * 1024 * 1024
        ),
    )(ensemble, flat(obs_value), flat(obs_error), flat(obs_index), obs_count.reshape(1, -1))


def solution(mesh):
    return jax.shard_map(
        functools.partial(local, mesh.shape["member"], mesh.shape["region"]),
        mesh=mesh,
        in_specs=(
            P("member", "region", None, None),
            P(None, ("member", "region"), None),
            P(None, ("member", "region"), None),
            P(None, ("member", "region"), None),
            P(None, ("member", "region")),
        ),
        out_specs=P("member", "region", None, None),
        check_vma=False,
    )
```

```python
import functools
import math

import jax
import jax.numpy as jnp
from jax import lax
from jax.experimental import pallas as pl
from jax.experimental.pallas import tpu as pltpu
from jax.sharding import PartitionSpec as P

SIDE = 16
CELLS = SIDE * SIDE
HALF = SIDE // 2
LANES = 128
SUB = 8
NS_ITERS = 6
LOC_SCALE = 12.0
INFLATION_FACTOR = 1.1
MESH = pl.DeviceIdType.MESH
NT = (((1,), (1,)), ((), ()))
T = 8
PHASES = 2
OWN = 128
ROW_HALO = 32
SIDE_HALO = 16
TARGETS = 256


def split(values):
    high = values.astype(jnp.bfloat16)
    low = (values - high.astype(jnp.float32)).astype(jnp.bfloat16)
    return high, low


def row_of(k, jb):
    kb = k // SUB
    return (0, 192, 320)[kb] + (k - SUB * kb) * (24 - SUB * kb) + SUB * (jb - kb)


def kernel(
    dims,
    ens_ref, value_any, error_any, index_any, count_ref, out_ref,
    value_ref, error_ref, index_ref, ens, pack, obs, slots, place, lochi, loclo, qhi, qlo, own, hin,
    halo_out, row_in, side_in, yfull, zfull, step, ypack, zpack, drv, half_ref, wt, xt, mean, outgoing, seam_tile, seam_out, seam_in,
    ens_send, ens_recv, obs_send, obs_recv, halo_send, halo_recv, out_send, out_recv, local_sem, own_sem, entry_sem,
    seam_send, seam_recv,
):
    M, G, K, R, V, O = dims
    members = M * K
    blocks = members // SUB
    PACKED = own.shape[0]
    m = lax.axis_index("member")
    g = lax.axis_index("region")
    f32 = jnp.float32

    loads = []
    for n, (src, dst) in enumerate(((value_any, value_ref), (error_any, error_ref), (index_any, index_ref))):
        load = pltpu.make_async_copy(src, dst, local_sem.at[n])
        load.start()
        loads.append(load)

    def tile(p, d):
        return pl.ds(pl.multiple_of((p * M + d) * T, T), T)

    def own_copy(p):
        return pltpu.make_async_copy(
            ens_ref.at[:, :, tile(p, m), :], ens.at[p, pl.ds(m * K, K)], own_sem.at[p]
        )

    for p in range(PHASES):
        own_copy(p).start()
    seam_load = pltpu.make_async_copy(ens_ref.at[:, :, tile(1, 0), :], seam_tile, local_sem.at[3])
    seam_load.start()

    column = m * G + g
    col_tile = column // T
    col_owner = lax.rem(col_tile, M)
    col_phase = col_tile // M
    col_at = lax.rem(column, T)
    holders = []
    for s in range(PHASES * T):
        c = ((s // T) * M + m) * T + s % T
        holders.append((c // G, lax.rem(c, G)))

    ring = 4
    y, z = lax.rem(g, ring), g // ring
    x_peers = [(lax.rem(m + off, M), g) for off in range(1, M)]
    y_peers = [(m, z * ring + lax.rem(y + off, ring)) for off in range(1, ring)]
    z_peers = [(m, lax.rem(g + off * ring, G)) for off in range(1, G // ring)]
    barrier = pltpu.get_barrier_semaphore()
    for peer in x_peers + y_peers + z_peers:
        pl.semaphore_signal(barrier, inc=1, device_id=peer, device_id_type=MESH)
    up_ok = g > 0
    down_ok = g < G - 1
    row_ok = {-1: up_ok, 1: down_ok}
    seam_load.wait()
    tiles = V // LANES
    seam_rows = tiles * SUB
    seam_out[...] = jnp.zeros(seam_out.shape, f32)
    for i in range(R):
        for k in range(K):
            for t in range(tiles):
                at = t * SUB + i * (SUB // R) + k
                seam_out[at : at + 1, :] = seam_tile[k, i, 0:1, t * LANES : (t + 1) * LANES]

    def seam_copy(source):
        return pltpu.make_async_remote_copy(
            src_ref=seam_out, dst_ref=seam_in.at[pl.ds(pl.multiple_of(source * seam_rows, SUB), seam_rows)],
            send_sem=seam_send.at[0], recv_sem=seam_recv.at[source],
            device_id=(0, g), device_id_type=MESH,
        )

    @pl.when(m == 0)
    def _():
        seam_in[:seam_rows, :] = seam_out[...]

    pl.semaphore_wait(barrier, len(x_peers) + len(y_peers) + len(z_peers))
    for peer in y_peers:
        pl.semaphore_signal(entry_sem.at[0], inc=1, device_id=peer, device_id_type=MESH)

    pieces = (((0, 2), (2, K)), ((0, 1), (1, K)))

    def ens_copy(p, n, off, to, at):
        a, b = pieces[p][n]
        return pltpu.make_async_remote_copy(
            src_ref=ens_ref.at[a:b, :, tile(p, to), :],
            dst_ref=ens.at[p, pl.ds(at * K + a, b - a)],
            send_sem=ens_send.at[p, n, off], recv_sem=ens_recv.at[p, n, off],
            device_id=(to, g), device_id_type=MESH,
        )

    order = [4, 5, 3, 2, 6, 1, 7]
    order = [off for off in order if off < M] + [off for off in range(1, M) if off not in order]
    @pl.when(m != 0)
    def _():
        seam_copy(m).start()

    for off in order:
        ens_copy(0, 0, off, lax.rem(m + off, M), m).start()
    pl.semaphore_wait(entry_sem.at[0], len(y_peers))
    for peer in x_peers:
        pl.semaphore_signal(entry_sem.at[1], inc=1, device_id=peer, device_id_type=MESH)

    for load in loads:
        load.wait()
    slot = lax.broadcasted_iota(jnp.int32, (G * R, O), 1)
    slot_row = lax.broadcasted_iota(jnp.int32, (G * R, O), 0)
    count = jnp.zeros((G * R, O), jnp.int32)
    for d in range(G * R):
        count = jnp.where(slot_row == d, count_ref[0, d], count)
    live = jnp.where(slot < count, 1.0, 0.0).astype(f32)
    weight = jnp.sqrt(live / error_ref[...])
    value = value_ref[...]
    index_f = index_ref[...].astype(f32)
    for d in range(G):
        base = d * SUB
        pack[base : base + R, :] = weight[d * R : (d + 1) * R]
        pack[base + R : base + 2 * R, :] = value[d * R : (d + 1) * R]
        pack[base + 2 * R : base + 3 * R, :] = index_f[d * R : (d + 1) * R]
        pack[base + 3 * R : base + SUB, :] = jnp.zeros((SUB - 3 * R, O), f32)
    used = OWN + 2 * ROW_HALO
    lochi[used:, :] = jnp.zeros((TARGETS - used, lochi.shape[1]), jnp.bfloat16)
    loclo[used:, :] = jnp.zeros((TARGETS - used, lochi.shape[1]), jnp.bfloat16)

    pl.semaphore_wait(entry_sem.at[1], len(x_peers))

    def obs_copy(to_m, to_g, src_g, p, e):
        return pltpu.make_async_remote_copy(
            src_ref=pack.at[pl.ds(pl.multiple_of(src_g * SUB, SUB), SUB)],
            dst_ref=obs.at[p, pl.ds(pl.multiple_of(e * SUB, SUB), SUB)],
            send_sem=obs_send.at[src_g], recv_sem=obs_recv.at[p, e],
            device_id=(to_m, to_g), device_id_type=MESH,
        )

    for off in range(1, G):
        to = lax.rem(g + off, G)
        obs_copy(col_owner, to, to, col_phase, col_at).start()

    @pl.when(col_owner != m)
    def _():
        obs_copy(col_owner, g, g, col_phase, col_at).start()

    @pl.when(col_owner == m)
    def _():
        obs[col_phase, pl.ds(pl.multiple_of(col_at * SUB, SUB), SUB), :] = pack[
            pl.ds(pl.multiple_of(g * SUB, SUB), SUB), :
        ]

    for p, n in ((0, 1), (1, 0)):
        for off in order:
            ens_copy(p, n, off, lax.rem(m + off, M), m).start()
    for s, (hm, hg) in enumerate(holders):
        @pl.when(jnp.logical_not(jnp.logical_and(hm == m, hg == g)))
        def _():
            obs_copy(hm, hg, g, s // T, s % T).wait_recv()

    def wait_ens(p):
        own_copy(p).wait()
        for n in range(2):
            for off in range(1, M):
                came = lax.rem(m + M - off, M)
                ens_copy(p, n, off, came, came).wait_recv()

    def gather(p):
        for i in range(R):
            wgt = obs[p, pl.ds(i, T, stride=SUB), :]
            val = obs[p, pl.ds(R + i, T, stride=SUB), :]
            idx = obs[p, pl.ds(2 * R + i, T, stride=SUB), :].astype(jnp.int32)
            lane = idx & (LANES - 1)
            which = idx >> 7
            cell = idx & (CELLS - 1)
            place[2 * i] = (cell >> 4).astype(f32)
            place[2 * i + 1] = (cell & (SIDE - 1)).astype(f32)
            seen = []
            for k in range(members):
                got = jnp.take_along_axis(ens[p, k, i, :, :LANES], lane, axis=1)
                for t in range(1, tiles):
                    more = jnp.take_along_axis(ens[p, k, i, :, t * LANES : (t + 1) * LANES], lane, axis=1)
                    got = jnp.where(which == t, more, got)
                seen.append(got)
            total = seen[0]
            for k in range(1, members):
                total = total + seen[k]
            avg = total * (1.0 / members)
            for k in range(members):
                slots[i, k * T : (k + 1) * T, :] = wgt * (seen[k] - avg)
            slots[i, members * T : (members + 1) * T, :] = wgt * (val - avg)

    def gather_seam():
        for n in range(1, M):
            seam_copy(n).wait_recv()
        for i in range(R):
            wgt = obs[1, i : i + 1, :]
            val = obs[1, R + i : R + i + 1, :]
            idx = obs[1, 2 * R + i : 2 * R + i + 1, :].astype(jnp.int32)
            cell = idx & (CELLS - 1)
            place[2 * i, 0:1, :] = (cell >> 4).astype(f32)
            place[2 * i + 1, 0:1, :] = (cell & (SIDE - 1)).astype(f32)
            wide = jnp.broadcast_to(idx, (M, O))
            lane = wide & (LANES - 1)
            which = wide >> 7
            seen = []
            for k in range(K):
                got = None
                for t in range(tiles):
                    rows = seam_in[pl.ds(t * SUB + i * (SUB // R) + k, M, stride=seam_rows), :]
                    more = jnp.take_along_axis(rows, lane, axis=1)
                    got = more if got is None else jnp.where(which == t, more, got)
                seen.append(got)
            total = seen[0]
            for k in range(1, K):
                total = total + seen[k]
            avg = jnp.sum(total, axis=0, keepdims=True) * (1.0 / members)
            for k in range(K):
                slots[i, pl.ds(k * T, M, stride=K * T), :] = wgt * (seen[k] - avg)
            slots[i, members * T : members * T + 1, :] = wgt * (val - avg)

    sub8 = lax.broadcasted_iota(jnp.int32, (SUB, O), 0)

    def products(c, i):
        at = (c * R + i) * O
        here = [slots[i, pl.ds(c + b * SUB * T, SUB, stride=T), :] for b in range(blocks)]
        innov = slots[i, members * T + c : members * T + c + 1, :]
        rows = []
        for k in range(members):
            kb = k // SUB
            left = here[kb][k % SUB : k % SUB + 1]
            for jb in range(kb, blocks):
                right = here[jb]
                use = left
                if jb == kb and k % SUB == SUB - 1:
                    use = jnp.where(sub8 < SUB - 1, innov, left)
                if jb == kb and k % SUB == SUB - 2:
                    use = jnp.where(sub8 < 1, innov, left)
                    right = jnp.where(sub8 < 1, right[SUB - 1 : SUB], right)
                rows.append(use * right)
        for n in range(0, len(rows), 2):
            high, low = split(jnp.concatenate(rows[n : n + 2], axis=0))
            qhi[n * SUB : (n + 2) * SUB, at : at + O] = high
            qlo[n * SUB : (n + 2) * SUB, at : at + O] = low

    scale = -1.0 / (2.0 * LOC_SCALE * LOC_SCALE)
    middle = (HALF - 1) * 0.5
    t_id = lax.broadcasted_iota(jnp.int32, (SUB, O), 0)
    t_row = t_id >> 1
    t_mid = (t_id & 1).astype(f32) * HALF + middle
    col = lax.broadcasted_iota(jnp.int32, (T, O), 0)

    def row_weight(c, i):
        y = place[2 * i, c : c + 1, :]
        row_off = i + 1 - t_row
        dy = (row_off * SIDE).astype(f32) + y - t_mid
        return jnp.where(jnp.abs(row_off) <= 1, jnp.exp(dy * dy * scale), 0.0)

    def edge_weight(c, i, ly, away):
        x = place[2 * i + 1, c : c + 1, :]
        parts = []
        for pc in range(2):
            dx = away * SIDE + x - (pc * HALF + middle)
            parts.append(ly * jnp.exp(dx * dx * scale))
        return jnp.concatenate(parts, axis=0)

    def locality(c, i):
        at = (c * R + i) * O
        x = place[2 * i + 1, c : c + 1, :]
        ly = row_weight(c, i)
        col_off = c - col
        lx = []
        for pc in range(2):
            dx = (col_off * SIDE).astype(f32) + x - (pc * HALF + middle)
            lx.append(jnp.where(jnp.abs(col_off) <= 1, jnp.exp(dx * dx * scale), 0.0))

        def put(first, values):
            high, low = split(values)
            for at_row in first:
                lochi[at_row : at_row + values.shape[0], at : at + O] = high
                loclo[at_row : at_row + values.shape[0], at : at + O] = low

        for pc in range(2):
            for it in range(R):
                s = 2 * (it + 1)
                pair = jnp.concatenate([ly[s : s + 1] * lx[pc], ly[s + 1 : s + 2] * lx[pc]], axis=0)
                first = (pc * R + it) * 2 * T
                put((first, OWN // 2 + first), pair)
            for n, s in enumerate((0, 2 * (R + 1))):
                pair = jnp.concatenate([ly[s : s + 1] * lx[pc], ly[s + 1 : s + 2] * lx[pc]], axis=0)
                put((OWN + n * ROW_HALO + pc * 2 * T,), pair)
        if c == 0:
            put((used,), edge_weight(c, i, ly, 1))
        if c == T - 1:
            put((used + SIDE_HALO,), edge_weight(c, i, ly, -1))

    def dot(left, right):
        return lax.dot_general(left, right, NT, preferred_element_type=f32)

    def halo_plan(p, dm, dg):
        n = (dm + 1) * 3 + dg + 1
        send = row_ok[dg] if dg else jnp.bool_(True)
        recv = row_ok[-dg] if dg else jnp.bool_(True)
        at = p
        if dm == 0:
            first = 0 if dg < 0 else ROW_HALO
            src = halo_out.at[p, pl.ds(first, ROW_HALO)]
            dst = row_in.at[p, 0 if dg < 0 else 1]
            come = p
        else:
            if dm < 0:
                send = jnp.logical_and(send, jnp.logical_or(m > 0, p == 0))
                recv = jnp.logical_and(recv, jnp.logical_or(m < M - 1, p == 0))
            else:
                send = jnp.logical_and(send, jnp.logical_or(m < M - 1, p == 0))
                recv = jnp.logical_and(recv, jnp.logical_or(m > 0, p == 1))
                at = jnp.where(m == M - 1, 1, p)
            first = 2 * ROW_HALO + (0 if dm < 0 else SIDE_HALO)
            src = halo_out.at[p, pl.ds(first, SIDE_HALO)]
            base = (0 if dm < 0 else 3) + dg + 1
            dst = side_in.at[at, base]
            come = p

        def copy(slot, to_m, to_g):
            target = row_in.at[slot, 0 if dg < 0 else 1] if dm == 0 else side_in.at[slot, (0 if dm < 0 else 3) + dg + 1]
            return pltpu.make_async_remote_copy(
                src_ref=src, dst_ref=target, send_sem=halo_send.at[p, n], recv_sem=halo_recv.at[slot, n],
                device_id=(to_m, to_g), device_id_type=MESH,
            )

        outward = lambda: copy(at, lax.rem(m + M + dm, M), g + dg)
        inward = lambda: copy(p, lax.rem(m + M - dm, M), g - dg)
        landing = row_in.at[p, 0 if dg < 0 else 1] if dm == 0 else side_in.at[p, (0 if dm < 0 else 3) + dg + 1]
        return send, recv, outward, inward, landing

    near = [(dm, dg) for dm in (0, 1, -1) for dg in (-1, 0, 1) if (dm, dg) != (0, 0)]
    lane = lax.broadcasted_iota(jnp.int32, (SUB, OWN), 1)
    west = (lane & 32) == 0
    sub = lax.broadcasted_iota(jnp.int32, (SUB, OWN), 0)

    front = lane < OWN // 2
    row_in_block = sub - jnp.where(front, 0, SUB // 2)
    quarter = SUB // 2

    def pack_rows(kb, r, jb, full):
        k = SUB * kb + r
        one = full[k * members + SUB * jb : k * members + SUB * (jb + 1), :]
        two = full[(k + quarter) * members + SUB * jb : (k + quarter) * members + SUB * (jb + 1), :]
        return jnp.where(front, one, two)

    def packed_at(kb, r, jb):
        at = (quarter * kb + r) * members + SUB * jb
        return slice(at, at + SUB)

    def square(left, right, full, packed, first=False):
        for kb in range(blocks):
            sums = {}
            for i in range(members):
                rights = [right[i * members + SUB * jb : i * members + SUB * (jb + 1), :] for jb in range(kb, blocks)]
                for r in range(quarter):
                    at = (quarter * kb + r) * members + i
                    lone = left[at : at + 1, :]
                    for jb in range(kb, blocks):
                        term = lone * rights[jb - kb]
                        sums[r, jb] = term if i == 0 else sums[r, jb] + term
            for r in range(quarter):
                for jb in range(kb, blocks):
                    out = sums[r, jb]
                    if first:
                        out = -0.5 * out
                        if jb == kb:
                            out = out + jnp.where(row_in_block == r, 1.5, 0.0)
                    swapped = pltpu.roll(out, OWN // 2, 1)
                    put_entry(full, SUB * kb + r, jb, jnp.where(front, out, swapped))
                    put_entry(full, SUB * kb + quarter + r, jb, jnp.where(front, swapped, out))
                    if packed is not None:
                        packed[packed_at(kb, r, jb), :] = out
                if packed is not None:
                    for jb in range(kb):
                        packed[packed_at(kb, r, jb), :] = pack_rows(kb, r, jb, full)

    def put_entry(into, k, jb, out):
        into[k * members + SUB * jb : k * members + SUB * (jb + 1), :] = out
        if jb > k // SUB:
            into[pl.ds(SUB * jb * members + k, SUB, stride=members), :] = out

    fields = V // CELLS
    halves = CELLS // LANES

    def results(p):
        chips = M // 2
        group = 2 * K

        def update(q, carry):
            away_chip = jnp.where(q == 0, chips // 2, jnp.where(q == chips - 1, 0, jnp.where(q == 1, 1, chips - 1)))
            chip = lax.rem(m // 2 + away_chip, chips)
            k0 = chip * group
            for pair in range(0, group, 2):
                sums = [[mean[r * SUB : (r + 1) * SUB, :] for r in range(SUB)] for _ in range(2)]
                for j in range(members):
                    lines = [xt[j, r * SUB : (r + 1) * SUB, :] for r in range(SUB)]
                    for e in range(2):
                        lone = wt[k0 + pair + e, j : j + 1, :]
                        sums[e] = [s + lone * line for s, line in zip(sums[e], lines)]
                rows = []
                for r in range(SUB):
                    one, two = sums[0][r], sums[1][r]
                    rows.append(jnp.where(west, one, pltpu.roll(two, 32, 1)))
                    rows.append(jnp.where(west, pltpu.roll(one, OWN - 32, 1), two))
                turned = jnp.transpose(jnp.concatenate(rows, axis=0))
                at = 0
                for f in range(fields):
                    for e in range(2):
                        for i in range(R):
                            for h in range(halves):
                                lanes = f * CELLS + h * LANES
                                outgoing[p, k0 + pair + e, i, :, lanes : lanes + LANES] = turned[at : at + T]
                                at += T
            for core in range(2):
                dest = 2 * chip + core
                away = lax.rem(dest - m + M, M)

                @pl.when(away != 0)
                def _():
                    out_copy(p, away, dest, m).start()

                @pl.when(away == 0)
                def _():
                    out_ref[:, :, tile(p, m), :] = outgoing[p, pl.ds(dest * K, K)]
            return carry

        lax.fori_loop(0, chips, update, 0)

    def phase(p, carry):
        first_phase = p == 0

        for n in range(PHASES):
            @pl.when(p == n)
            def _():
                wait_ens(n)

        gather(p)
        for c in range(T):
            for i in range(R):
                products(c, i)
                locality(c, i)
        both = dot(qhi[...], lochi[...]) + dot(qhi[...], loclo[...]) + dot(qlo[...], lochi[...])
        own[...] = both[:, :OWN]
        halo_out[p] = jnp.transpose(both[:, OWN:])[: halo_out.shape[1]]

        plans = [halo_plan(p, dm, dg) for dm, dg in near]
        for (dm, dg), (send, recv, outward, inward, landing) in zip(near, plans):
            if dm >= 0:
                @pl.when(send)
                def _():
                    outward().start()

        @pl.when(jnp.logical_and(first_phase, m == 0))
        def _():
            gather_seam()
            edges = []
            for i in range(R):
                products(0, i)
                edges.append(edge_weight(0, i, row_weight(0, i), 1))
            high, low = split(jnp.concatenate(edges, axis=1))
            seam = qhi[:, : R * O]
            halo_out[0, 2 * ROW_HALO : 2 * ROW_HALO + SIDE_HALO, :] = (
                dot(high, seam) + dot(low, seam) + dot(high, qlo[:, : R * O])
            )

        for (dm, dg), (send, recv, outward, inward, landing) in zip(near, plans):
            if dm < 0:
                @pl.when(send)
                def _():
                    outward().start()

        @pl.when(first_phase)
        def _():
            for off in order:
                ens_copy(1, 1, off, lax.rem(m + off, M), m).start()

        @pl.when(p > 0)
        def _():
            results(p - 1)

        total = None
        for k in range(members):
            rows = []
            for f in range(fields):
                part = [
                    ens[p, k, i, :, f * CELLS + h * LANES : f * CELLS + (h + 1) * LANES]
                    for i in range(R) for h in range(halves)
                ]
                rows += part + part
            turned = jnp.transpose(jnp.concatenate(rows, axis=0))
            lines = []
            for r in range(SUB):
                lines.append(jnp.where(west, turned[16 * r : 16 * r + 8], turned[16 * r + 8 : 16 * r + 16]))
            for r in range(SUB):
                xt[k, r * SUB : (r + 1) * SUB, :] = lines[r]
            total = lines if total is None else [a + b for a, b in zip(total, lines)]
        avg = [line * (1.0 / members) for line in total]
        for r in range(SUB):
            mean[r * SUB : (r + 1) * SUB, :] = avg[r]
        for k in range(members):
            for r in range(SUB):
                xt[k, r * SUB : (r + 1) * SUB, :] = xt[k, r * SUB : (r + 1) * SUB, :] - avg[r]

        for send, recv, outward, inward, landing in plans:
            @pl.when(recv)
            def _():
                inward().wait_recv()

            @pl.when(jnp.logical_not(recv))
            def _():
                landing[...] = jnp.zeros(landing.shape, f32)

        col8 = lax.broadcasted_iota(jnp.int32, (T, PACKED), 0)
        for pc in range(2):
            for i in range(R):
                for pr in range(2):
                    at = (pc * 2 + pr) * T
                    block = None
                    if i == R - 1:
                        block = row_in[p, 0, at : at + T, :]
                    if i == 0:
                        more = row_in[p, 1, at : at + T, :]
                        block = more if block is None else block + more
                    for base, at_col in ((0, T - 1), (3, 0)):
                        def pick(dg, t):
                            place_in = pc * SUB + t * 2 + pr
                            return side_in[p, base + dg + 1, place_in : place_in + 1, :]

                        line = pick(0, i + 1)
                        if i == R - 1:
                            line = line + pick(-1, 0)
                        if i == 0:
                            line = line + pick(1, R + 1)
                        more = jnp.where(col8 == at_col, line, 0.0)
                        block = more if block is None else block + more
                    at = ((pc * R + i) * 2 + pr) * T
                    hin[at : at + T, :] = block
                    hin[OWN // 2 + at : OWN // 2 + at + T, :] = block
        prec = own[...] + jnp.transpose(hin[...])

        for b in range(blocks):
            top = prec[row_of(SUB * b + SUB - 1, b) : row_of(SUB * b + SUB - 1, b) + SUB]
            last = prec[row_of(SUB * b + SUB - 2, b) : row_of(SUB * b + SUB - 2, b) + 1]
            drv[SUB * b : SUB * (b + 1), :] = jnp.where(sub < SUB - 1, top, last)
        inflate = (members - 1) / INFLATION_FACTOR
        for k in range(members):
            kb = k // SUB
            for jb in range(kb, blocks):
                out = prec[row_of(k, jb) : row_of(k, jb) + SUB]
                if jb == kb:
                    keep = {SUB - 1: sub >= SUB - 1, SUB - 2: sub >= 1}.get(k % SUB)
                    if keep is not None:
                        out = jnp.where(keep, out, 0.0)
                    out = out + jnp.where(sub == k % SUB, inflate, 0.0)
                put_entry(yfull, k, jb, out)
        for b in range(blocks):
            for e in (SUB - 1, SUB - 2):
                k = SUB * b + e
                yfull[k * members + SUB * b : k * members + SUB * (b + 1), :] = yfull[
                    pl.ds(SUB * b * members + k, SUB, stride=members), :
                ]
        squares = None
        for n in range(members * blocks):
            line = yfull[n * SUB : (n + 1) * SUB, :]
            squares = line * line if squares is None else squares + line * line
        norm = jnp.sqrt(jnp.sum(squares, axis=0, keepdims=True))
        small = 1.0 / norm
        for k in range(members):
            for jb in range(blocks):
                rows = slice(k * members + SUB * jb, k * members + SUB * (jb + 1))
                start = yfull[rows, :] * small
                first_m = -0.5 * start
                if jb == k // SUB:
                    first_m = first_m + jnp.where(sub == k % SUB, 1.5, 0.0)
                yfull[rows, :] = start
                step[rows, :] = first_m
        for kb in range(blocks):
            for r in range(quarter):
                for jb in range(blocks):
                    ypack[packed_at(kb, r, jb), :] = pack_rows(kb, r, jb, yfull)
                    zpack[packed_at(kb, r, jb), :] = pack_rows(kb, r, jb, step)
        square(ypack, step, yfull, ypack)

        def sweep(n, carry):
            square(zpack, yfull, step, None, True)
            square(ypack, step, yfull, ypack)
            square(zpack, step, zfull, zpack)
            return carry

        lax.fori_loop(0, NS_ITERS - 2, sweep, 0)
        square(zpack, yfull, step, None, True)
        square(zpack, step, zfull, None)

        shrink = 1.0 / jnp.sqrt(norm)

        def applied(vector):
            sums = [None] * blocks
            for i in range(members):
                lone = vector[i : i + 1, :]
                for jb in range(blocks):
                    term = lone * zfull[i * members + SUB * jb : i * members + SUB * (jb + 1), :]
                    sums[jb] = term if i == 0 else sums[jb] + term
            return [line * shrink for line in sums]

        for jb, line in enumerate(applied(drv)):
            half_ref[SUB * jb : SUB * (jb + 1), :] = line
        mean_w = applied(half_ref)
        spread = math.sqrt(members - 1) * shrink
        for k in range(members):
            for jb in range(blocks):
                wt[k, SUB * jb : SUB * (jb + 1), :] = (
                    mean_w[jb] + spread * zfull[k * members + SUB * jb : k * members + SUB * (jb + 1), :]
                )

        return carry

    def out_copy(p, away, dest, source):
        return pltpu.make_async_remote_copy(
            src_ref=outgoing.at[p, pl.ds(dest * K, K)],
            dst_ref=out_ref.at[:, :, tile(p, source), :],
            send_sem=out_send.at[p, away], recv_sem=out_recv.at[p, away],
            device_id=(dest, g), device_id_type=MESH,
        )

    lax.fori_loop(0, PHASES, phase, 0)
    results(PHASES - 1)

    for off in range(1, G):
        to = lax.rem(g + off, G)
        obs_copy(col_owner, to, to, col_phase, col_at).wait_send()

    @pl.when(col_owner != m)
    def _():
        obs_copy(col_owner, g, g, col_phase, col_at).wait_send()

    @pl.when(m != 0)
    def _():
        seam_copy(m).wait_send()

    for p in range(PHASES):
        for n in range(2):
            for off in range(1, M):
                ens_copy(p, n, off, lax.rem(m + off, M), m).wait_send()
        for dm, dg in near:
            send, recv, outward, inward, landing = halo_plan(p, dm, dg)

            @pl.when(send)
            def _():
                outward().wait_send()
    for p in range(PHASES):
        for off in range(1, M):
            out_copy(p, off, lax.rem(m + off, M), m).wait_send()
            out_copy(p, off, m, lax.rem(m + M - off, M)).wait_recv()


def local(M, G, ensemble, obs_value, obs_error, obs_index, obs_count):
    K, R, cols, V = ensemble.shape
    O = obs_value.shape[2]
    members = M * K
    assert cols == PHASES * M * T and cols == M * G and R == 2 and members == 24 and V == 2 * CELLS and O == LANES
    wide = T * R * O
    packed = 384
    square = members * members
    f32 = jnp.float32
    vmem = pltpu.VMEM
    dma = pltpu.SemaphoreType.DMA
    flat = lambda a: a.reshape(a.shape[0], -1)
    return pl.pallas_call(
        functools.partial(kernel, (M, G, K, R, V, O)),
        out_shape=pltpu.VMEM(ensemble.shape, f32),
        in_specs=[pl.BlockSpec(memory_space=pl.ANY)] * 4
        + [pl.BlockSpec(memory_space=pltpu.SMEM)],
        out_specs=pl.BlockSpec(memory_space=vmem),
        scratch_shapes=[
            vmem((G * R, O), f32),
            vmem((G * R, O), f32),
            vmem((G * R, O), jnp.int32),
            vmem((PHASES, members, R, T, V), f32),
            vmem((G * SUB, O), f32),
            vmem((PHASES, T * SUB, O), f32),
            vmem((R, (members + 1) * T, O), f32),
            vmem((2 * R, T, O), f32),
            vmem((TARGETS, wide), jnp.bfloat16),
            vmem((TARGETS, wide), jnp.bfloat16),
            vmem((packed, wide), jnp.bfloat16),
            vmem((packed, wide), jnp.bfloat16),
            vmem((packed, OWN), f32),
            vmem((OWN, packed), f32),
            vmem((PHASES, 2 * ROW_HALO + 2 * SIDE_HALO, packed), f32),
            vmem((PHASES, 2, ROW_HALO, packed), f32),
            vmem((PHASES, 6, SIDE_HALO, packed), f32),
            vmem((square, OWN), f32),
            vmem((square, OWN), f32),
            vmem((square, OWN), f32),
            vmem((square // 2, OWN), f32),
            vmem((square // 2, OWN), f32),
            vmem((members, OWN), f32),
            vmem((members, OWN), f32),
            vmem((members, members, OWN), f32),
            vmem((members, SUB * SUB, OWN), f32),
            vmem((SUB * SUB, OWN), f32),
            vmem((PHASES, members, R, T, V), f32),
            vmem((K, R, T, V), f32),
            vmem((V // LANES * SUB, LANES), f32),
            vmem((M * (V // LANES) * SUB, LANES), f32),
            dma((PHASES, 2, M)), dma((PHASES, 2, M)), dma((G,)), dma((PHASES, T)),
            dma((PHASES, 9)), dma((PHASES, 9)), dma((PHASES, M)), dma((PHASES, M)), dma((4,)), dma((PHASES,)),
            pltpu.SemaphoreType.REGULAR((2,)),
            dma((1,)), dma((M,)),
        ],
        compiler_params=pltpu.CompilerParams(
            collective_id=0, has_side_effects=True, vmem_limit_bytes=56 * 1024 * 1024
        ),
    )(ensemble, flat(obs_value), flat(obs_error), flat(obs_index), obs_count.reshape(1, -1))


def solution(mesh):
    return jax.shard_map(
        functools.partial(local, mesh.shape["member"], mesh.shape["region"]),
        mesh=mesh,
        in_specs=(
            P("member", "region", None, None),
            P(None, ("member", "region"), None),
            P(None, ("member", "region"), None),
            P(None, ("member", "region"), None),
            P(None, ("member", "region")),
        ),
        out_specs=P("member", "region", None, None),
        check_vma=False,
    )
```

```python
import functools
import math

import jax
import jax.numpy as jnp
from jax import lax
from jax.experimental import pallas as pl
from jax.experimental.pallas import tpu as pltpu
from jax.sharding import PartitionSpec as P

SIDE = 16
CELLS = SIDE * SIDE
HALF = SIDE // 2
LANES = 128
SUB = 8
NS_ITERS = 6
LOC_SCALE = 12.0
INFLATION_FACTOR = 1.1
MESH = pl.DeviceIdType.MESH
NT = (((1,), (1,)), ((), ()))
T = 8
PHASES = 2
OWN = 128
ROW_HALO = 32
SIDE_HALO = 16
TARGETS = 256


def split(values):
    high = values.astype(jnp.bfloat16)
    low = (values - high.astype(jnp.float32)).astype(jnp.bfloat16)
    return high, low


def row_of(k, jb):
    kb = k // SUB
    return (0, 192, 320)[kb] + (k - SUB * kb) * (24 - SUB * kb) + SUB * (jb - kb)


def kernel(
    dims,
    ens_ref, value_any, error_any, index_any, count_ref, out_ref,
    value_ref, error_ref, index_ref, ens, pack, obs, slots, place, lochi, loclo, qhi, qlo, own, hin,
    halo_out, row_in, side_in, yfull, zfull, step, ypack, zpack, drv, half_ref, wt, xt, mean, outgoing, seam_tile, seam_out, seam_in, seam_side,
    ens_send, ens_recv, obs_send, obs_recv, halo_send, halo_recv, out_send, out_recv, local_sem, own_sem, entry_sem,
    seam_send, seam_recv,
):
    M, G, K, R, V, O = dims
    members = M * K
    blocks = members // SUB
    PACKED = own.shape[0]
    m = lax.axis_index("member")
    g = lax.axis_index("region")
    f32 = jnp.float32

    loads = []
    for n, (src, dst) in enumerate(((value_any, value_ref), (error_any, error_ref), (index_any, index_ref))):
        load = pltpu.make_async_copy(src, dst, local_sem.at[n])
        load.start()
        loads.append(load)

    def tile(p, d):
        return pl.ds(pl.multiple_of((p * M + d) * T, T), T)

    def own_copy(p):
        return pltpu.make_async_copy(
            ens_ref.at[:, :, tile(p, m), :], ens.at[p, pl.ds(m * K, K)], own_sem.at[p]
        )

    for p in range(PHASES):
        own_copy(p).start()
    seam_load = pltpu.make_async_copy(ens_ref.at[:, :, tile(1, 0), :], seam_tile, local_sem.at[3])
    seam_load.start()

    column = m * G + g
    col_tile = column // T
    col_owner = lax.rem(col_tile, M)
    col_phase = col_tile // M
    col_at = lax.rem(column, T)
    holders = []
    for s in range(PHASES * T):
        c = ((s // T) * M + m) * T + s % T
        holders.append((c // G, lax.rem(c, G)))

    ring = 4
    y, z = lax.rem(g, ring), g // ring
    x_peers = [(lax.rem(m + off, M), g) for off in range(1, M)]
    y_peers = [(m, z * ring + lax.rem(y + off, ring)) for off in range(1, ring)]
    z_peers = [(m, lax.rem(g + off * ring, G)) for off in range(1, G // ring)]
    barrier = pltpu.get_barrier_semaphore()
    for peer in x_peers + y_peers + z_peers:
        pl.semaphore_signal(barrier, inc=1, device_id=peer, device_id_type=MESH)
    up_ok = g > 0
    down_ok = g < G - 1
    row_ok = {-1: up_ok, 1: down_ok}
    seam_load.wait()
    tiles = V // LANES
    seam_rows = tiles * SUB
    seam_out[...] = jnp.zeros(seam_out.shape, f32)
    for i in range(R):
        for k in range(K):
            for t in range(tiles):
                at = t * SUB + i * (SUB // R) + k
                seam_out[at : at + 1, :] = seam_tile[k, i, 0:1, t * LANES : (t + 1) * LANES]

    def seam_copy(source):
        return pltpu.make_async_remote_copy(
            src_ref=seam_out, dst_ref=seam_in.at[pl.ds(pl.multiple_of(source * seam_rows, SUB), seam_rows)],
            send_sem=seam_send.at[0], recv_sem=seam_recv.at[source],
            device_id=(0, g), device_id_type=MESH,
        )

    @pl.when(m == 0)
    def _():
        seam_in[:seam_rows, :] = seam_out[...]

    pl.semaphore_wait(barrier, len(x_peers) + len(y_peers) + len(z_peers))
    for peer in y_peers:
        pl.semaphore_signal(entry_sem.at[0], inc=1, device_id=peer, device_id_type=MESH)

    pieces = (((0, 2), (2, K)), ((0, 1), (1, K)))

    def ens_copy(p, n, off, to, at):
        a, b = pieces[p][n]
        return pltpu.make_async_remote_copy(
            src_ref=ens_ref.at[a:b, :, tile(p, to), :],
            dst_ref=ens.at[p, pl.ds(at * K + a, b - a)],
            send_sem=ens_send.at[p, n, off], recv_sem=ens_recv.at[p, n, off],
            device_id=(to, g), device_id_type=MESH,
        )

    order = [4, 5, 3, 2, 6, 1, 7]
    order = [off for off in order if off < M] + [off for off in range(1, M) if off not in order]
    @pl.when(m != 0)
    def _():
        seam_copy(m).start()

    for off in order:
        ens_copy(0, 0, off, lax.rem(m + off, M), m).start()
    pl.semaphore_wait(entry_sem.at[0], len(y_peers))
    for peer in x_peers:
        pl.semaphore_signal(entry_sem.at[1], inc=1, device_id=peer, device_id_type=MESH)

    for load in loads:
        load.wait()
    slot = lax.broadcasted_iota(jnp.int32, (G * R, O), 1)
    slot_row = lax.broadcasted_iota(jnp.int32, (G * R, O), 0)
    count = jnp.zeros((G * R, O), jnp.int32)
    for d in range(G * R):
        count = jnp.where(slot_row == d, count_ref[0, d], count)
    live = jnp.where(slot < count, 1.0, 0.0).astype(f32)
    weight = jnp.sqrt(live / error_ref[...])
    value = value_ref[...]
    index_f = index_ref[...].astype(f32)
    for d in range(G):
        base = d * SUB
        pack[base : base + R, :] = weight[d * R : (d + 1) * R]
        pack[base + R : base + 2 * R, :] = value[d * R : (d + 1) * R]
        pack[base + 2 * R : base + 3 * R, :] = index_f[d * R : (d + 1) * R]
        pack[base + 3 * R : base + SUB, :] = jnp.zeros((SUB - 3 * R, O), f32)
    used = OWN + 2 * ROW_HALO
    lochi[used:, :] = jnp.zeros((TARGETS - used, lochi.shape[1]), jnp.bfloat16)
    loclo[used:, :] = jnp.zeros((TARGETS - used, lochi.shape[1]), jnp.bfloat16)

    pl.semaphore_wait(entry_sem.at[1], len(x_peers))

    def obs_copy(to_m, to_g, src_g, p, e):
        return pltpu.make_async_remote_copy(
            src_ref=pack.at[pl.ds(pl.multiple_of(src_g * SUB, SUB), SUB)],
            dst_ref=obs.at[p, pl.ds(pl.multiple_of(e * SUB, SUB), SUB)],
            send_sem=obs_send.at[src_g], recv_sem=obs_recv.at[p, e],
            device_id=(to_m, to_g), device_id_type=MESH,
        )

    for off in range(1, G):
        to = lax.rem(g + off, G)
        obs_copy(col_owner, to, to, col_phase, col_at).start()

    @pl.when(col_owner != m)
    def _():
        obs_copy(col_owner, g, g, col_phase, col_at).start()

    @pl.when(col_owner == m)
    def _():
        obs[col_phase, pl.ds(pl.multiple_of(col_at * SUB, SUB), SUB), :] = pack[
            pl.ds(pl.multiple_of(g * SUB, SUB), SUB), :
        ]

    for p, n in ((0, 1), (1, 0)):
        for off in order:
            ens_copy(p, n, off, lax.rem(m + off, M), m).start()
    def wait_obs(s, also):
        hm, hg = holders[s]

        @pl.when(jnp.logical_and(also, jnp.logical_not(jnp.logical_and(hm == m, hg == g))))
        def _():
            obs_copy(hm, hg, g, s // T, s % T).wait_recv()

    for s in range(T):
        wait_obs(s, jnp.bool_(True))

    def wait_ens(p):
        own_copy(p).wait()
        for n in range(2):
            for off in range(1, M):
                came = lax.rem(m + M - off, M)
                ens_copy(p, n, off, came, came).wait_recv()

    def gather(p):
        for i in range(R):
            wgt = obs[p, pl.ds(i, T, stride=SUB), :]
            val = obs[p, pl.ds(R + i, T, stride=SUB), :]
            idx = obs[p, pl.ds(2 * R + i, T, stride=SUB), :].astype(jnp.int32)
            lane = idx & (LANES - 1)
            which = idx >> 7
            cell = idx & (CELLS - 1)
            place[2 * i] = (cell >> 4).astype(f32)
            place[2 * i + 1] = (cell & (SIDE - 1)).astype(f32)
            seen = []
            for k in range(members):
                got = jnp.take_along_axis(ens[p, k, i, :, :LANES], lane, axis=1)
                for t in range(1, tiles):
                    more = jnp.take_along_axis(ens[p, k, i, :, t * LANES : (t + 1) * LANES], lane, axis=1)
                    got = jnp.where(which == t, more, got)
                seen.append(got)
            total = seen[0]
            for k in range(1, members):
                total = total + seen[k]
            avg = total * (1.0 / members)
            for k in range(members):
                slots[i, k * T : (k + 1) * T, :] = wgt * (seen[k] - avg)
            slots[i, members * T : (members + 1) * T, :] = wgt * (val - avg)

    def gather_seam():
        for n in range(1, M):
            seam_copy(n).wait_recv()
        for i in range(R):
            wgt = obs[1, i : i + 1, :]
            val = obs[1, R + i : R + i + 1, :]
            idx = obs[1, 2 * R + i : 2 * R + i + 1, :].astype(jnp.int32)
            cell = idx & (CELLS - 1)
            place[2 * i, 0:1, :] = (cell >> 4).astype(f32)
            place[2 * i + 1, 0:1, :] = (cell & (SIDE - 1)).astype(f32)
            wide = jnp.broadcast_to(idx, (M, O))
            lane = wide & (LANES - 1)
            which = wide >> 7
            seen = []
            for k in range(K):
                got = None
                for t in range(tiles):
                    rows = seam_in[pl.ds(t * SUB + i * (SUB // R) + k, M, stride=seam_rows), :]
                    more = jnp.take_along_axis(rows, lane, axis=1)
                    got = more if got is None else jnp.where(which == t, more, got)
                seen.append(got)
            total = seen[0]
            for k in range(1, K):
                total = total + seen[k]
            avg = jnp.sum(total, axis=0, keepdims=True) * (1.0 / members)
            for k in range(K):
                slots[i, pl.ds(k * T, M, stride=K * T), :] = wgt * (seen[k] - avg)
            slots[i, members * T : members * T + 1, :] = wgt * (val - avg)

    sub8 = lax.broadcasted_iota(jnp.int32, (SUB, O), 0)

    def products(c, i):
        at = (c * R + i) * O
        here = [slots[i, pl.ds(c + b * SUB * T, SUB, stride=T), :] for b in range(blocks)]
        innov = slots[i, members * T + c : members * T + c + 1, :]
        rows = []
        for k in range(members):
            kb = k // SUB
            left = here[kb][k % SUB : k % SUB + 1]
            for jb in range(kb, blocks):
                right = here[jb]
                use = left
                if jb == kb and k % SUB == SUB - 1:
                    use = jnp.where(sub8 < SUB - 1, innov, left)
                if jb == kb and k % SUB == SUB - 2:
                    use = jnp.where(sub8 < 1, innov, left)
                    right = jnp.where(sub8 < 1, right[SUB - 1 : SUB], right)
                rows.append(use * right)
        for n in range(0, len(rows), 2):
            high, low = split(jnp.concatenate(rows[n : n + 2], axis=0))
            qhi[n * SUB : (n + 2) * SUB, at : at + O] = high
            qlo[n * SUB : (n + 2) * SUB, at : at + O] = low

    scale = -1.0 / (2.0 * LOC_SCALE * LOC_SCALE)
    middle = (HALF - 1) * 0.5
    t_id = lax.broadcasted_iota(jnp.int32, (SUB, O), 0)
    t_row = t_id >> 1
    t_mid = (t_id & 1).astype(f32) * HALF + middle
    col = lax.broadcasted_iota(jnp.int32, (T, O), 0)

    def row_weight(c, i):
        y = place[2 * i, c : c + 1, :]
        row_off = i + 1 - t_row
        dy = (row_off * SIDE).astype(f32) + y - t_mid
        return jnp.where(jnp.abs(row_off) <= 1, jnp.exp(dy * dy * scale), 0.0)

    def edge_weight(c, i, ly, away):
        x = place[2 * i + 1, c : c + 1, :]
        parts = []
        for pc in range(2):
            dx = away * SIDE + x - (pc * HALF + middle)
            parts.append(ly * jnp.exp(dx * dx * scale))
        return jnp.concatenate(parts, axis=0)

    def locality(c, i):
        at = (c * R + i) * O
        x = place[2 * i + 1, c : c + 1, :]
        ly = row_weight(c, i)
        col_off = c - col
        lx = []
        for pc in range(2):
            dx = (col_off * SIDE).astype(f32) + x - (pc * HALF + middle)
            lx.append(jnp.where(jnp.abs(col_off) <= 1, jnp.exp(dx * dx * scale), 0.0))

        def put(first, values):
            high, low = split(values)
            for at_row in first:
                lochi[at_row : at_row + values.shape[0], at : at + O] = high
                loclo[at_row : at_row + values.shape[0], at : at + O] = low

        for pc in range(2):
            for it in range(R):
                s = 2 * (it + 1)
                pair = jnp.concatenate([ly[s : s + 1] * lx[pc], ly[s + 1 : s + 2] * lx[pc]], axis=0)
                first = (pc * R + it) * 2 * T
                put((first, OWN // 2 + first), pair)
            for n, s in enumerate((0, 2 * (R + 1))):
                pair = jnp.concatenate([ly[s : s + 1] * lx[pc], ly[s + 1 : s + 2] * lx[pc]], axis=0)
                put((OWN + n * ROW_HALO + pc * 2 * T,), pair)
        if c == 0:
            put((used,), edge_weight(c, i, ly, 1))
        if c == T - 1:
            put((used + SIDE_HALO,), edge_weight(c, i, ly, -1))

    def dot(left, right):
        return lax.dot_general(left, right, NT, preferred_element_type=f32)

    def halo_plan(p, dm, dg):
        n = (dm + 1) * 3 + dg + 1
        send = row_ok[dg] if dg else jnp.bool_(True)
        recv = row_ok[-dg] if dg else jnp.bool_(True)
        at = p
        if dm == 0:
            first = 0 if dg < 0 else ROW_HALO
            src = halo_out.at[p, pl.ds(first, ROW_HALO)]
            dst = row_in.at[p, 0 if dg < 0 else 1]
            come = p
        else:
            if dm < 0:
                send = jnp.logical_and(send, jnp.logical_or(m > 0, p == 0))
                recv = jnp.logical_and(recv, jnp.logical_or(m < M - 1, p == 0))
            else:
                send = jnp.logical_and(send, jnp.logical_or(m < M - 1, p == 0))
                recv = jnp.logical_and(recv, jnp.logical_or(m > 0, p == 1))
                at = jnp.where(m == M - 1, 1, p)
            first = 2 * ROW_HALO + (0 if dm < 0 else SIDE_HALO)
            src = halo_out.at[p, pl.ds(first, SIDE_HALO)]
            base = (0 if dm < 0 else 3) + dg + 1
            dst = side_in.at[at, base]
            come = p

        def copy(slot, to_m, to_g):
            target = row_in.at[slot, 0 if dg < 0 else 1] if dm == 0 else side_in.at[slot, (0 if dm < 0 else 3) + dg + 1]
            return pltpu.make_async_remote_copy(
                src_ref=src, dst_ref=target, send_sem=halo_send.at[p, n], recv_sem=halo_recv.at[slot, n],
                device_id=(to_m, to_g), device_id_type=MESH,
            )

        outward = lambda: copy(at, lax.rem(m + M + dm, M), g + dg)
        inward = lambda: copy(p, lax.rem(m + M - dm, M), g - dg)
        landing = row_in.at[p, 0 if dg < 0 else 1] if dm == 0 else side_in.at[p, (0 if dm < 0 else 3) + dg + 1]
        return send, recv, outward, inward, landing

    near = [(dm, dg) for dm in (0, 1, -1) for dg in (-1, 0, 1) if (dm, dg) != (0, 0)]
    lane = lax.broadcasted_iota(jnp.int32, (SUB, OWN), 1)
    west = (lane & 32) == 0
    sub = lax.broadcasted_iota(jnp.int32, (SUB, OWN), 0)

    front = lane < OWN // 2
    row_in_block = sub - jnp.where(front, 0, SUB // 2)
    quarter = SUB // 2

    def pack_rows(kb, r, jb, full):
        k = SUB * kb + r
        one = full[k * members + SUB * jb : k * members + SUB * (jb + 1), :]
        two = full[(k + quarter) * members + SUB * jb : (k + quarter) * members + SUB * (jb + 1), :]
        return jnp.where(front, one, two)

    def packed_at(kb, r, jb):
        at = (quarter * kb + r) * members + SUB * jb
        return slice(at, at + SUB)

    def square(left, right, full, packed, first=False):
        for kb in range(blocks):
            sums = {}
            for i in range(members):
                rights = [right[i * members + SUB * jb : i * members + SUB * (jb + 1), :] for jb in range(kb, blocks)]
                for r in range(quarter):
                    at = (quarter * kb + r) * members + i
                    lone = left[at : at + 1, :]
                    for jb in range(kb, blocks):
                        term = lone * rights[jb - kb]
                        sums[r, jb] = term if i == 0 else sums[r, jb] + term
            for r in range(quarter):
                for jb in range(kb, blocks):
                    out = sums[r, jb]
                    if first:
                        out = -0.5 * out
                        if jb == kb:
                            out = out + jnp.where(row_in_block == r, 1.5, 0.0)
                    swapped = pltpu.roll(out, OWN // 2, 1)
                    put_entry(full, SUB * kb + r, jb, jnp.where(front, out, swapped))
                    put_entry(full, SUB * kb + quarter + r, jb, jnp.where(front, swapped, out))
                    if packed is not None:
                        packed[packed_at(kb, r, jb), :] = out
                if packed is not None:
                    for jb in range(kb):
                        packed[packed_at(kb, r, jb), :] = pack_rows(kb, r, jb, full)

    def put_entry(into, k, jb, out):
        into[k * members + SUB * jb : k * members + SUB * (jb + 1), :] = out
        if jb > k // SUB:
            into[pl.ds(SUB * jb * members + k, SUB, stride=members), :] = out

    fields = V // CELLS
    halves = CELLS // LANES

    def results(p):
        chips = M // 2
        group = 2 * K

        def update(q, carry):
            away_chip = jnp.where(q == 0, chips // 2, jnp.where(q == chips - 1, 0, jnp.where(q == 1, 1, chips - 1)))
            chip = lax.rem(m // 2 + away_chip, chips)
            k0 = chip * group
            for pair in range(0, group, 2):
                sums = [[mean[r * SUB : (r + 1) * SUB, :] for r in range(SUB)] for _ in range(2)]
                for j in range(members):
                    lines = [xt[j, r * SUB : (r + 1) * SUB, :] for r in range(SUB)]
                    for e in range(2):
                        lone = wt[k0 + pair + e, j : j + 1, :]
                        sums[e] = [s + lone * line for s, line in zip(sums[e], lines)]
                rows = []
                for r in range(SUB):
                    one, two = sums[0][r], sums[1][r]
                    rows.append(jnp.where(west, one, pltpu.roll(two, 32, 1)))
                    rows.append(jnp.where(west, pltpu.roll(one, OWN - 32, 1), two))
                turned = jnp.transpose(jnp.concatenate(rows, axis=0))
                at = 0
                for f in range(fields):
                    for e in range(2):
                        for i in range(R):
                            for h in range(halves):
                                lanes = f * CELLS + h * LANES
                                outgoing[p, k0 + pair + e, i, :, lanes : lanes + LANES] = turned[at : at + T]
                                at += T
            for core in range(2):
                dest = 2 * chip + core
                away = lax.rem(dest - m + M, M)

                @pl.when(away != 0)
                def _():
                    out_copy(p, away, dest, m).start()

                @pl.when(away == 0)
                def _():
                    out_ref[:, :, tile(p, m), :] = outgoing[p, pl.ds(dest * K, K)]
            return carry

        lax.fori_loop(0, chips, update, 0)

    def phase(p, carry):
        first_phase = p == 0

        for n in range(PHASES):
            @pl.when(p == n)
            def _():
                wait_ens(n)

        for s in range(T, PHASES * T):
            wait_obs(s, jnp.logical_and(p == 1, m != 0) if s == T else p == 1)
        gather(p)
        for c in range(T):
            for i in range(R):
                products(c, i)
                locality(c, i)
        both = dot(qhi[...], lochi[...]) + dot(qhi[...], loclo[...]) + dot(qlo[...], lochi[...])
        own[...] = both[:, :OWN]
        halo_out[p] = jnp.transpose(both[:, OWN:])[: halo_out.shape[1]]


        @pl.when(jnp.logical_and(first_phase, m == 0))
        def _():
            halo_out[0, 2 * ROW_HALO : 2 * ROW_HALO + SIDE_HALO, :] = seam_side[...]

        plans = [halo_plan(p, dm, dg) for dm, dg in near]
        for (dm, dg), (send, recv, outward, inward, landing) in zip(near, plans):
            @pl.when(send)
            def _():
                outward().start()

        @pl.when(first_phase)
        def _():
            for off in order:
                ens_copy(1, 1, off, lax.rem(m + off, M), m).start()

        @pl.when(p > 0)
        def _():
            results(p - 1)

        total = None
        for k in range(members):
            rows = []
            for f in range(fields):
                part = [
                    ens[p, k, i, :, f * CELLS + h * LANES : f * CELLS + (h + 1) * LANES]
                    for i in range(R) for h in range(halves)
                ]
                rows += part + part
            turned = jnp.transpose(jnp.concatenate(rows, axis=0))
            lines = []
            for r in range(SUB):
                lines.append(jnp.where(west, turned[16 * r : 16 * r + 8], turned[16 * r + 8 : 16 * r + 16]))
            for r in range(SUB):
                xt[k, r * SUB : (r + 1) * SUB, :] = lines[r]
            total = lines if total is None else [a + b for a, b in zip(total, lines)]
        avg = [line * (1.0 / members) for line in total]
        for r in range(SUB):
            mean[r * SUB : (r + 1) * SUB, :] = avg[r]
        for k in range(members):
            for r in range(SUB):
                xt[k, r * SUB : (r + 1) * SUB, :] = xt[k, r * SUB : (r + 1) * SUB, :] - avg[r]

        for send, recv, outward, inward, landing in plans:
            @pl.when(recv)
            def _():
                inward().wait_recv()

            @pl.when(jnp.logical_not(recv))
            def _():
                landing[...] = jnp.zeros(landing.shape, f32)

        col8 = lax.broadcasted_iota(jnp.int32, (T, PACKED), 0)
        for pc in range(2):
            for i in range(R):
                for pr in range(2):
                    at = (pc * 2 + pr) * T
                    block = None
                    if i == R - 1:
                        block = row_in[p, 0, at : at + T, :]
                    if i == 0:
                        more = row_in[p, 1, at : at + T, :]
                        block = more if block is None else block + more
                    for base, at_col in ((0, T - 1), (3, 0)):
                        def pick(dg, t):
                            place_in = pc * SUB + t * 2 + pr
                            return side_in[p, base + dg + 1, place_in : place_in + 1, :]

                        line = pick(0, i + 1)
                        if i == R - 1:
                            line = line + pick(-1, 0)
                        if i == 0:
                            line = line + pick(1, R + 1)
                        more = jnp.where(col8 == at_col, line, 0.0)
                        block = more if block is None else block + more
                    at = ((pc * R + i) * 2 + pr) * T
                    hin[at : at + T, :] = block
                    hin[OWN // 2 + at : OWN // 2 + at + T, :] = block
        prec = own[...] + jnp.transpose(hin[...])

        for b in range(blocks):
            top = prec[row_of(SUB * b + SUB - 1, b) : row_of(SUB * b + SUB - 1, b) + SUB]
            last = prec[row_of(SUB * b + SUB - 2, b) : row_of(SUB * b + SUB - 2, b) + 1]
            drv[SUB * b : SUB * (b + 1), :] = jnp.where(sub < SUB - 1, top, last)
        inflate = (members - 1) / INFLATION_FACTOR
        for k in range(members):
            kb = k // SUB
            for jb in range(kb, blocks):
                out = prec[row_of(k, jb) : row_of(k, jb) + SUB]
                if jb == kb:
                    keep = {SUB - 1: sub >= SUB - 1, SUB - 2: sub >= 1}.get(k % SUB)
                    if keep is not None:
                        out = jnp.where(keep, out, 0.0)
                    out = out + jnp.where(sub == k % SUB, inflate, 0.0)
                put_entry(yfull, k, jb, out)
        for b in range(blocks):
            for e in (SUB - 1, SUB - 2):
                k = SUB * b + e
                yfull[k * members + SUB * b : k * members + SUB * (b + 1), :] = yfull[
                    pl.ds(SUB * b * members + k, SUB, stride=members), :
                ]
        squares = None
        for n in range(members * blocks):
            line = yfull[n * SUB : (n + 1) * SUB, :]
            squares = line * line if squares is None else squares + line * line
        norm = jnp.sqrt(jnp.sum(squares, axis=0, keepdims=True))
        small = 1.0 / norm
        for k in range(members):
            for jb in range(blocks):
                rows = slice(k * members + SUB * jb, k * members + SUB * (jb + 1))
                start = yfull[rows, :] * small
                first_m = -0.5 * start
                if jb == k // SUB:
                    first_m = first_m + jnp.where(sub == k % SUB, 1.5, 0.0)
                yfull[rows, :] = start
                step[rows, :] = first_m
        for kb in range(blocks):
            for r in range(quarter):
                for jb in range(blocks):
                    ypack[packed_at(kb, r, jb), :] = pack_rows(kb, r, jb, yfull)
                    zpack[packed_at(kb, r, jb), :] = pack_rows(kb, r, jb, step)
        square(ypack, step, yfull, ypack)

        def sweep(n, carry):
            square(zpack, yfull, step, None, True)
            square(ypack, step, yfull, ypack)
            square(zpack, step, zfull, zpack)
            return carry

        lax.fori_loop(0, NS_ITERS - 2, sweep, 0, unroll=True)
        square(zpack, yfull, step, None, True)
        square(zpack, step, zfull, None)

        shrink = 1.0 / jnp.sqrt(norm)

        def applied(vector):
            sums = [None] * blocks
            for i in range(members):
                lone = vector[i : i + 1, :]
                for jb in range(blocks):
                    term = lone * zfull[i * members + SUB * jb : i * members + SUB * (jb + 1), :]
                    sums[jb] = term if i == 0 else sums[jb] + term
            return [line * shrink for line in sums]

        for jb, line in enumerate(applied(drv)):
            half_ref[SUB * jb : SUB * (jb + 1), :] = line
        mean_w = applied(half_ref)
        spread = math.sqrt(members - 1) * shrink
        for k in range(members):
            for jb in range(blocks):
                wt[k, SUB * jb : SUB * (jb + 1), :] = (
                    mean_w[jb] + spread * zfull[k * members + SUB * jb : k * members + SUB * (jb + 1), :]
                )

        return carry

    def out_copy(p, away, dest, source):
        return pltpu.make_async_remote_copy(
            src_ref=outgoing.at[p, pl.ds(dest * K, K)],
            dst_ref=out_ref.at[:, :, tile(p, source), :],
            send_sem=out_send.at[p, away], recv_sem=out_recv.at[p, away],
            device_id=(dest, g), device_id_type=MESH,
        )

    wait_obs(T, m == 0)

    @pl.when(m == 0)
    def _():
        gather_seam()
        edges = []
        for i in range(R):
            products(0, i)
            edges.append(edge_weight(0, i, row_weight(0, i), 1))
        high, low = split(jnp.concatenate(edges, axis=1))
        seam = qhi[:, : R * O]
        seam_side[...] = dot(high, seam) + dot(low, seam) + dot(high, qlo[:, : R * O])

    lax.fori_loop(0, PHASES, phase, 0)
    results(PHASES - 1)

    for off in range(1, G):
        to = lax.rem(g + off, G)
        obs_copy(col_owner, to, to, col_phase, col_at).wait_send()

    @pl.when(col_owner != m)
    def _():
        obs_copy(col_owner, g, g, col_phase, col_at).wait_send()

    @pl.when(m != 0)
    def _():
        seam_copy(m).wait_send()

    for p in range(PHASES):
        for n in range(2):
            for off in range(1, M):
                ens_copy(p, n, off, lax.rem(m + off, M), m).wait_send()
        for dm, dg in near:
            send, recv, outward, inward, landing = halo_plan(p, dm, dg)

            @pl.when(send)
            def _():
                outward().wait_send()
    for p in range(PHASES):
        for off in range(1, M):
            out_copy(p, off, lax.rem(m + off, M), m).wait_send()
            out_copy(p, off, m, lax.rem(m + M - off, M)).wait_recv()


def local(M, G, ensemble, obs_value, obs_error, obs_index, obs_count):
    K, R, cols, V = ensemble.shape
    O = obs_value.shape[2]
    members = M * K
    assert cols == PHASES * M * T and cols == M * G and R == 2 and members == 24 and V == 2 * CELLS and O == LANES
    wide = T * R * O
    packed = 384
    square = members * members
    f32 = jnp.float32
    vmem = pltpu.VMEM
    dma = pltpu.SemaphoreType.DMA
    flat = lambda a: a.reshape(a.shape[0], -1)
    return pl.pallas_call(
        functools.partial(kernel, (M, G, K, R, V, O)),
        out_shape=pltpu.VMEM(ensemble.shape, f32),
        in_specs=[pl.BlockSpec(memory_space=pl.ANY)] * 4
        + [pl.BlockSpec(memory_space=pltpu.SMEM)],
        out_specs=pl.BlockSpec(memory_space=vmem),
        scratch_shapes=[
            vmem((G * R, O), f32),
            vmem((G * R, O), f32),
            vmem((G * R, O), jnp.int32),
            vmem((PHASES, members, R, T, V), f32),
            vmem((G * SUB, O), f32),
            vmem((PHASES, T * SUB, O), f32),
            vmem((R, (members + 1) * T, O), f32),
            vmem((2 * R, T, O), f32),
            vmem((TARGETS, wide), jnp.bfloat16),
            vmem((TARGETS, wide), jnp.bfloat16),
            vmem((packed, wide), jnp.bfloat16),
            vmem((packed, wide), jnp.bfloat16),
            vmem((packed, OWN), f32),
            vmem((OWN, packed), f32),
            vmem((PHASES, 2 * ROW_HALO + 2 * SIDE_HALO, packed), f32),
            vmem((PHASES, 2, ROW_HALO, packed), f32),
            vmem((PHASES, 6, SIDE_HALO, packed), f32),
            vmem((square, OWN), f32),
            vmem((square, OWN), f32),
            vmem((square, OWN), f32),
            vmem((square // 2, OWN), f32),
            vmem((square // 2, OWN), f32),
            vmem((members, OWN), f32),
            vmem((members, OWN), f32),
            vmem((members, members, OWN), f32),
            vmem((members, SUB * SUB, OWN), f32),
            vmem((SUB * SUB, OWN), f32),
            vmem((PHASES, members, R, T, V), f32),
            vmem((K, R, T, V), f32),
            vmem((V // LANES * SUB, LANES), f32),
            vmem((M * (V // LANES) * SUB, LANES), f32),
            vmem((SIDE_HALO, packed), f32),
            dma((PHASES, 2, M)), dma((PHASES, 2, M)), dma((G,)), dma((PHASES, T)),
            dma((PHASES, 9)), dma((PHASES, 9)), dma((PHASES, M)), dma((PHASES, M)), dma((4,)), dma((PHASES,)),
            pltpu.SemaphoreType.REGULAR((2,)),
            dma((1,)), dma((M,)),
        ],
        compiler_params=pltpu.CompilerParams(
            collective_id=0, has_side_effects=True, vmem_limit_bytes=56 * 1024 * 1024
        ),
    )(ensemble, flat(obs_value), flat(obs_error), flat(obs_index), obs_count.reshape(1, -1))


def solution(mesh):
    return jax.shard_map(
        functools.partial(local, mesh.shape["member"], mesh.shape["region"]),
        mesh=mesh,
        in_specs=(
            P("member", "region", None, None),
            P(None, ("member", "region"), None),
            P(None, ("member", "region"), None),
            P(None, ("member", "region"), None),
            P(None, ("member", "region")),
        ),
        out_specs=P("member", "region", None, None),
        check_vma=False,
    )
```

```python
import functools
import math

import jax
import jax.numpy as jnp
from jax import lax
from jax.experimental import pallas as pl
from jax.experimental.pallas import tpu as pltpu
from jax.sharding import PartitionSpec as P

SIDE = 16
CELLS = SIDE * SIDE
HALF = SIDE // 2
LANES = 128
SUB = 8
NS_ITERS = 6
LOC_SCALE = 12.0
INFLATION_FACTOR = 1.1
MESH = pl.DeviceIdType.MESH
NT = (((1,), (1,)), ((), ()))
T = 8
PHASES = 2
OWN = 128
ROW_HALO = 32
SIDE_HALO = 16
TARGETS = 256


def split(values):
    high = values.astype(jnp.bfloat16)
    low = (values - high.astype(jnp.float32)).astype(jnp.bfloat16)
    return high, low


def row_of(k, jb):
    kb = k // SUB
    return (0, 192, 320)[kb] + (k - SUB * kb) * (24 - SUB * kb) + SUB * (jb - kb)


def kernel(
    dims,
    ens_ref, value_any, error_any, index_any, count_ref, out_ref,
    value_ref, error_ref, index_ref, ens, pack, obs, slots, place, lochi, loclo, qhi, qlo, own, hin,
    halo_out, row_in, side_in, yfull, zfull, step, ypack, zpack, drv, half_ref, wt, xt, mean, outgoing, seam_tile, seam_out, seam_in, seam_side,
    ens_send, ens_recv, obs_send, obs_recv, halo_send, halo_recv, out_send, out_recv, local_sem, own_sem, entry_sem,
    seam_send, seam_recv,
):
    M, G, K, R, V, O = dims
    members = M * K
    blocks = members // SUB
    PACKED = own.shape[0]
    m = lax.axis_index("member")
    g = lax.axis_index("region")
    f32 = jnp.float32

    loads = []
    for n, (src, dst) in enumerate(((value_any, value_ref), (error_any, error_ref), (index_any, index_ref))):
        load = pltpu.make_async_copy(src, dst, local_sem.at[n])
        load.start()
        loads.append(load)

    def tile(p, d):
        return pl.ds(pl.multiple_of((p * M + d) * T, T), T)

    def own_copy(p):
        return pltpu.make_async_copy(
            ens_ref.at[:, :, tile(p, m), :], ens.at[p, pl.ds(m * K, K)], own_sem.at[p]
        )

    for p in range(PHASES):
        own_copy(p).start()
    seam_load = pltpu.make_async_copy(ens_ref.at[:, :, tile(1, 0), :], seam_tile, local_sem.at[3])
    seam_load.start()

    column = m * G + g
    col_tile = column // T
    col_owner = lax.rem(col_tile, M)
    col_phase = col_tile // M
    col_at = lax.rem(column, T)
    holders = []
    for s in range(PHASES * T):
        c = ((s // T) * M + m) * T + s % T
        holders.append((c // G, lax.rem(c, G)))

    ring = 4
    y, z = lax.rem(g, ring), g // ring
    x_peers = [(lax.rem(m + off, M), g) for off in range(1, M)]
    y_peers = [(m, z * ring + lax.rem(y + off, ring)) for off in range(1, ring)]
    z_peers = [(m, lax.rem(g + off * ring, G)) for off in range(1, G // ring)]
    barrier = pltpu.get_barrier_semaphore()
    for peer in x_peers + y_peers + z_peers:
        pl.semaphore_signal(barrier, inc=1, device_id=peer, device_id_type=MESH)
    up_ok = g > 0
    down_ok = g < G - 1
    row_ok = {-1: up_ok, 1: down_ok}
    seam_load.wait()
    tiles = V // LANES
    seam_rows = tiles * SUB
    seam_out[...] = jnp.zeros(seam_out.shape, f32)
    for i in range(R):
        for k in range(K):
            for t in range(tiles):
                at = t * SUB + i * (SUB // R) + k
                seam_out[at : at + 1, :] = seam_tile[k, i, 0:1, t * LANES : (t + 1) * LANES]

    def seam_copy(source):
        return pltpu.make_async_remote_copy(
            src_ref=seam_out, dst_ref=seam_in.at[pl.ds(pl.multiple_of(source * seam_rows, SUB), seam_rows)],
            send_sem=seam_send.at[0], recv_sem=seam_recv.at[source],
            device_id=(0, g), device_id_type=MESH,
        )

    @pl.when(m == 0)
    def _():
        seam_in[:seam_rows, :] = seam_out[...]

    pl.semaphore_wait(barrier, len(x_peers) + len(y_peers) + len(z_peers))
    for peer in y_peers:
        pl.semaphore_signal(entry_sem.at[0], inc=1, device_id=peer, device_id_type=MESH)

    pieces = (((0, 2), (2, K)), ((0, 1), (1, K)))

    def ens_copy(p, n, off, to, at):
        a, b = pieces[p][n]
        return pltpu.make_async_remote_copy(
            src_ref=ens_ref.at[a:b, :, tile(p, to), :],
            dst_ref=ens.at[p, pl.ds(at * K + a, b - a)],
            send_sem=ens_send.at[p, n, off], recv_sem=ens_recv.at[p, n, off],
            device_id=(to, g), device_id_type=MESH,
        )

    order = [4, 5, 3, 2, 6, 1, 7]
    order = [off for off in order if off < M] + [off for off in range(1, M) if off not in order]
    @pl.when(m != 0)
    def _():
        seam_copy(m).start()

    for off in order:
        ens_copy(0, 0, off, lax.rem(m + off, M), m).start()
    pl.semaphore_wait(entry_sem.at[0], len(y_peers))
    for peer in x_peers:
        pl.semaphore_signal(entry_sem.at[1], inc=1, device_id=peer, device_id_type=MESH)

    for load in loads:
        load.wait()
    slot = lax.broadcasted_iota(jnp.int32, (G * R, O), 1)
    slot_row = lax.broadcasted_iota(jnp.int32, (G * R, O), 0)
    count = jnp.zeros((G * R, O), jnp.int32)
    for d in range(G * R):
        count = jnp.where(slot_row == d, count_ref[0, d], count)
    live = jnp.where(slot < count, 1.0, 0.0).astype(f32)
    weight = jnp.sqrt(live / error_ref[...])
    value = value_ref[...]
    index_f = index_ref[...].astype(f32)
    for d in range(G):
        base = d * SUB
        pack[base : base + R, :] = weight[d * R : (d + 1) * R]
        pack[base + R : base + 2 * R, :] = value[d * R : (d + 1) * R]
        pack[base + 2 * R : base + 3 * R, :] = index_f[d * R : (d + 1) * R]
        pack[base + 3 * R : base + SUB, :] = jnp.zeros((SUB - 3 * R, O), f32)
    used = OWN + 2 * ROW_HALO
    lochi[used:, :] = jnp.zeros((TARGETS - used, lochi.shape[1]), jnp.bfloat16)
    loclo[used:, :] = jnp.zeros((TARGETS - used, lochi.shape[1]), jnp.bfloat16)

    pl.semaphore_wait(entry_sem.at[1], len(x_peers))

    def obs_copy(to_m, to_g, src_g, p, e):
        return pltpu.make_async_remote_copy(
            src_ref=pack.at[pl.ds(pl.multiple_of(src_g * SUB, SUB), SUB)],
            dst_ref=obs.at[p, pl.ds(pl.multiple_of(e * SUB, SUB), SUB)],
            send_sem=obs_send.at[src_g], recv_sem=obs_recv.at[p, e],
            device_id=(to_m, to_g), device_id_type=MESH,
        )

    for off in range(1, G):
        to = lax.rem(g + off, G)
        obs_copy(col_owner, to, to, col_phase, col_at).start()

    @pl.when(col_owner != m)
    def _():
        obs_copy(col_owner, g, g, col_phase, col_at).start()

    @pl.when(col_owner == m)
    def _():
        obs[col_phase, pl.ds(pl.multiple_of(col_at * SUB, SUB), SUB), :] = pack[
            pl.ds(pl.multiple_of(g * SUB, SUB), SUB), :
        ]

    for p, n in ((0, 1), (1, 0)):
        for off in order:
            ens_copy(p, n, off, lax.rem(m + off, M), m).start()
    def wait_obs(s, also):
        hm, hg = holders[s]

        @pl.when(jnp.logical_and(also, jnp.logical_not(jnp.logical_and(hm == m, hg == g))))
        def _():
            obs_copy(hm, hg, g, s // T, s % T).wait_recv()

    for s in range(T):
        wait_obs(s, jnp.bool_(True))

    def wait_ens(p):
        own_copy(p).wait()
        for n in range(2):
            for off in range(1, M):
                came = lax.rem(m + M - off, M)
                ens_copy(p, n, off, came, came).wait_recv()

    def gather(p):
        for i in range(R):
            wgt = obs[p, pl.ds(i, T, stride=SUB), :]
            val = obs[p, pl.ds(R + i, T, stride=SUB), :]
            idx = obs[p, pl.ds(2 * R + i, T, stride=SUB), :].astype(jnp.int32)
            lane = idx & (LANES - 1)
            which = idx >> 7
            cell = idx & (CELLS - 1)
            place[2 * i] = (cell >> 4).astype(f32)
            place[2 * i + 1] = (cell & (SIDE - 1)).astype(f32)
            seen = []
            for k in range(members):
                got = jnp.take_along_axis(ens[p, k, i, :, :LANES], lane, axis=1)
                for t in range(1, tiles):
                    more = jnp.take_along_axis(ens[p, k, i, :, t * LANES : (t + 1) * LANES], lane, axis=1)
                    got = jnp.where(which == t, more, got)
                seen.append(got)
            total = seen[0]
            for k in range(1, members):
                total = total + seen[k]
            avg = total * (1.0 / members)
            for k in range(members):
                slots[i, k * T : (k + 1) * T, :] = wgt * (seen[k] - avg)
            slots[i, members * T : (members + 1) * T, :] = wgt * (val - avg)

    def gather_seam():
        for n in range(1, M):
            seam_copy(n).wait_recv()
        for i in range(R):
            wgt = obs[1, i : i + 1, :]
            val = obs[1, R + i : R + i + 1, :]
            idx = obs[1, 2 * R + i : 2 * R + i + 1, :].astype(jnp.int32)
            cell = idx & (CELLS - 1)
            place[2 * i, 0:1, :] = (cell >> 4).astype(f32)
            place[2 * i + 1, 0:1, :] = (cell & (SIDE - 1)).astype(f32)
            wide = jnp.broadcast_to(idx, (M, O))
            lane = wide & (LANES - 1)
            which = wide >> 7
            seen = []
            for k in range(K):
                got = None
                for t in range(tiles):
                    rows = seam_in[pl.ds(t * SUB + i * (SUB // R) + k, M, stride=seam_rows), :]
                    more = jnp.take_along_axis(rows, lane, axis=1)
                    got = more if got is None else jnp.where(which == t, more, got)
                seen.append(got)
            total = seen[0]
            for k in range(1, K):
                total = total + seen[k]
            avg = jnp.sum(total, axis=0, keepdims=True) * (1.0 / members)
            for k in range(K):
                slots[i, pl.ds(k * T, M, stride=K * T), :] = wgt * (seen[k] - avg)
            slots[i, members * T : members * T + 1, :] = wgt * (val - avg)

    sub8 = lax.broadcasted_iota(jnp.int32, (SUB, O), 0)

    def products(c, i):
        at = (c * R + i) * O
        here = [slots[i, pl.ds(c + b * SUB * T, SUB, stride=T), :] for b in range(blocks)]
        innov = slots[i, members * T + c : members * T + c + 1, :]
        rows = []
        for k in range(members):
            kb = k // SUB
            left = here[kb][k % SUB : k % SUB + 1]
            for jb in range(kb, blocks):
                right = here[jb]
                use = left
                if jb == kb and k % SUB == SUB - 1:
                    use = jnp.where(sub8 < SUB - 1, innov, left)
                if jb == kb and k % SUB == SUB - 2:
                    use = jnp.where(sub8 < 1, innov, left)
                    right = jnp.where(sub8 < 1, right[SUB - 1 : SUB], right)
                rows.append(use * right)
        for n in range(0, len(rows), 2):
            high, low = split(jnp.concatenate(rows[n : n + 2], axis=0))
            qhi[n * SUB : (n + 2) * SUB, at : at + O] = high
            qlo[n * SUB : (n + 2) * SUB, at : at + O] = low

    scale = -1.0 / (2.0 * LOC_SCALE * LOC_SCALE)
    middle = (HALF - 1) * 0.5
    t_id = lax.broadcasted_iota(jnp.int32, (SUB, O), 0)
    t_row = t_id >> 1
    t_mid = (t_id & 1).astype(f32) * HALF + middle
    col = lax.broadcasted_iota(jnp.int32, (T, O), 0)

    def row_weight(c, i):
        y = place[2 * i, c : c + 1, :]
        row_off = i + 1 - t_row
        dy = (row_off * SIDE).astype(f32) + y - t_mid
        return jnp.where(jnp.abs(row_off) <= 1, jnp.exp(dy * dy * scale), 0.0)

    def edge_weight(c, i, ly, away):
        x = place[2 * i + 1, c : c + 1, :]
        parts = []
        for pc in range(2):
            dx = away * SIDE + x - (pc * HALF + middle)
            parts.append(ly * jnp.exp(dx * dx * scale))
        return jnp.concatenate(parts, axis=0)

    def locality(c, i):
        at = (c * R + i) * O
        x = place[2 * i + 1, c : c + 1, :]
        ly = row_weight(c, i)
        col_off = c - col
        lx = []
        for pc in range(2):
            dx = (col_off * SIDE).astype(f32) + x - (pc * HALF + middle)
            lx.append(jnp.where(jnp.abs(col_off) <= 1, jnp.exp(dx * dx * scale), 0.0))

        def put(first, values):
            high, low = split(values)
            for at_row in first:
                lochi[at_row : at_row + values.shape[0], at : at + O] = high
                loclo[at_row : at_row + values.shape[0], at : at + O] = low

        for pc in range(2):
            for it in range(R):
                s = 2 * (it + 1)
                pair = jnp.concatenate([ly[s : s + 1] * lx[pc], ly[s + 1 : s + 2] * lx[pc]], axis=0)
                first = (pc * R + it) * 2 * T
                put((first, OWN // 2 + first), pair)
            for n, s in enumerate((0, 2 * (R + 1))):
                pair = jnp.concatenate([ly[s : s + 1] * lx[pc], ly[s + 1 : s + 2] * lx[pc]], axis=0)
                put((OWN + n * ROW_HALO + pc * 2 * T,), pair)
        if c == 0:
            put((used,), edge_weight(c, i, ly, 1))
        if c == T - 1:
            put((used + SIDE_HALO,), edge_weight(c, i, ly, -1))

    def dot(left, right):
        return lax.dot_general(left, right, NT, preferred_element_type=f32)

    def halo_plan(p, dm, dg):
        n = (dm + 1) * 3 + dg + 1
        send = row_ok[dg] if dg else jnp.bool_(True)
        recv = row_ok[-dg] if dg else jnp.bool_(True)
        at = p
        if dm == 0:
            first = 0 if dg < 0 else ROW_HALO
            src = halo_out.at[p, pl.ds(first, ROW_HALO)]
            dst = row_in.at[p, 0 if dg < 0 else 1]
            come = p
        else:
            if dm < 0:
                send = jnp.logical_and(send, jnp.logical_or(m > 0, p == 0))
                recv = jnp.logical_and(recv, jnp.logical_or(m < M - 1, p == 0))
            else:
                send = jnp.logical_and(send, jnp.logical_or(m < M - 1, p == 0))
                recv = jnp.logical_and(recv, jnp.logical_or(m > 0, p == 1))
                at = jnp.where(m == M - 1, 1, p)
            first = 2 * ROW_HALO + (0 if dm < 0 else SIDE_HALO)
            src = halo_out.at[p, pl.ds(first, SIDE_HALO)]
            base = (0 if dm < 0 else 3) + dg + 1
            dst = side_in.at[at, base]
            come = p

        def copy(slot, to_m, to_g):
            target = row_in.at[slot, 0 if dg < 0 else 1] if dm == 0 else side_in.at[slot, (0 if dm < 0 else 3) + dg + 1]
            return pltpu.make_async_remote_copy(
                src_ref=src, dst_ref=target, send_sem=halo_send.at[p, n], recv_sem=halo_recv.at[slot, n],
                device_id=(to_m, to_g), device_id_type=MESH,
            )

        outward = lambda: copy(at, lax.rem(m + M + dm, M), g + dg)
        inward = lambda: copy(p, lax.rem(m + M - dm, M), g - dg)
        landing = row_in.at[p, 0 if dg < 0 else 1] if dm == 0 else side_in.at[p, (0 if dm < 0 else 3) + dg + 1]
        return send, recv, outward, inward, landing

    near = [(dm, dg) for dm in (0, 1, -1) for dg in (-1, 0, 1) if (dm, dg) != (0, 0)]
    lane = lax.broadcasted_iota(jnp.int32, (SUB, OWN), 1)
    west = (lane & 32) == 0
    sub = lax.broadcasted_iota(jnp.int32, (SUB, OWN), 0)

    front = lane < OWN // 2
    row_in_block = sub - jnp.where(front, 0, SUB // 2)
    quarter = SUB // 2

    def pack_rows(kb, r, jb, full):
        k = SUB * kb + r
        one = full[k * members + SUB * jb : k * members + SUB * (jb + 1), :]
        two = full[(k + quarter) * members + SUB * jb : (k + quarter) * members + SUB * (jb + 1), :]
        return jnp.where(front, one, two)

    def packed_at(kb, r, jb):
        at = (quarter * kb + r) * members + SUB * jb
        return slice(at, at + SUB)

    def square(left, right, full, packed, first=False):
        for kb in range(blocks):
            sums = {}
            for i in range(members):
                rights = [right[i * members + SUB * jb : i * members + SUB * (jb + 1), :] for jb in range(kb, blocks)]
                for r in range(quarter):
                    at = (quarter * kb + r) * members + i
                    lone = left[at : at + 1, :]
                    for jb in range(kb, blocks):
                        term = lone * rights[jb - kb]
                        sums[r, jb] = term if i == 0 else sums[r, jb] + term
            for r in range(quarter):
                for jb in range(kb, blocks):
                    out = sums[r, jb]
                    if first:
                        out = -0.5 * out
                        if jb == kb:
                            out = out + jnp.where(row_in_block == r, 1.5, 0.0)
                    swapped = pltpu.roll(out, OWN // 2, 1)
                    put_entry(full, SUB * kb + r, jb, jnp.where(front, out, swapped))
                    put_entry(full, SUB * kb + quarter + r, jb, jnp.where(front, swapped, out))
                    if packed is not None:
                        packed[packed_at(kb, r, jb), :] = out
                if packed is not None:
                    for jb in range(kb):
                        packed[packed_at(kb, r, jb), :] = pack_rows(kb, r, jb, full)

    def put_entry(into, k, jb, out):
        into[k * members + SUB * jb : k * members + SUB * (jb + 1), :] = out
        if jb > k // SUB:
            into[pl.ds(SUB * jb * members + k, SUB, stride=members), :] = out

    fields = V // CELLS
    halves = CELLS // LANES

    def results(p):
        chips = M // 2
        group = 2 * K

        def update(q, carry):
            away_chip = jnp.where(q == 0, chips // 2, jnp.where(q == chips - 1, 0, jnp.where(q == 1, 1, chips - 1)))
            chip = lax.rem(m // 2 + away_chip, chips)
            k0 = chip * group
            for pair in range(0, group, 2):
                sums = [[mean[r * SUB : (r + 1) * SUB, :] for r in range(SUB)] for _ in range(2)]
                for j in range(members):
                    lines = [xt[j, r * SUB : (r + 1) * SUB, :] for r in range(SUB)]
                    for e in range(2):
                        lone = wt[k0 + pair + e, j : j + 1, :]
                        sums[e] = [s + lone * line for s, line in zip(sums[e], lines)]
                rows = []
                for r in range(SUB):
                    one, two = sums[0][r], sums[1][r]
                    rows.append(jnp.where(west, one, pltpu.roll(two, 32, 1)))
                    rows.append(jnp.where(west, pltpu.roll(one, OWN - 32, 1), two))
                turned = jnp.transpose(jnp.concatenate(rows, axis=0))
                at = 0
                for f in range(fields):
                    for e in range(2):
                        for i in range(R):
                            for h in range(halves):
                                lanes = f * CELLS + h * LANES
                                outgoing[p, k0 + pair + e, i, :, lanes : lanes + LANES] = turned[at : at + T]
                                at += T
                for core in ((), (0,), (1,))[pair // 2]:
                    dest = 2 * chip + core
                    away = lax.rem(dest - m + M, M)

                    @pl.when(away != 0)
                    def _():
                        out_copy(p, away, dest, m).start()

                    @pl.when(away == 0)
                    def _():
                        out_ref[:, :, tile(p, m), :] = outgoing[p, pl.ds(dest * K, K)]
            return carry

        lax.fori_loop(0, chips, update, 0)

    def phase(p, carry):
        first_phase = p == 0

        for n in range(PHASES):
            @pl.when(p == n)
            def _():
                wait_ens(n)

        for s in range(T, PHASES * T):
            wait_obs(s, jnp.logical_and(p == 1, m != 0) if s == T else p == 1)
        gather(p)
        for c in range(T):
            for i in range(R):
                products(c, i)
                locality(c, i)
        both = dot(qhi[...], lochi[...]) + dot(qhi[...], loclo[...]) + dot(qlo[...], lochi[...])
        own[...] = both[:, :OWN]
        halo_out[p] = jnp.transpose(both[:, OWN:])[: halo_out.shape[1]]


        @pl.when(jnp.logical_and(first_phase, m == 0))
        def _():
            halo_out[0, 2 * ROW_HALO : 2 * ROW_HALO + SIDE_HALO, :] = seam_side[...]

        plans = [halo_plan(p, dm, dg) for dm, dg in near]
        for (dm, dg), (send, recv, outward, inward, landing) in zip(near, plans):
            @pl.when(send)
            def _():
                outward().start()

        @pl.when(first_phase)
        def _():
            for off in order:
                ens_copy(1, 1, off, lax.rem(m + off, M), m).start()

        @pl.when(p > 0)
        def _():
            results(p - 1)

        total = None
        for k in range(members):
            rows = []
            for f in range(fields):
                part = [
                    ens[p, k, i, :, f * CELLS + h * LANES : f * CELLS + (h + 1) * LANES]
                    for i in range(R) for h in range(halves)
                ]
                rows += part + part
            turned = jnp.transpose(jnp.concatenate(rows, axis=0))
            lines = []
            for r in range(SUB):
                lines.append(jnp.where(west, turned[16 * r : 16 * r + 8], turned[16 * r + 8 : 16 * r + 16]))
            for r in range(SUB):
                xt[k, r * SUB : (r + 1) * SUB, :] = lines[r]
            total = lines if total is None else [a + b for a, b in zip(total, lines)]
        avg = [line * (1.0 / members) for line in total]
        for r in range(SUB):
            mean[r * SUB : (r + 1) * SUB, :] = avg[r]
        for k in range(members):
            for r in range(SUB):
                xt[k, r * SUB : (r + 1) * SUB, :] = xt[k, r * SUB : (r + 1) * SUB, :] - avg[r]

        for send, recv, outward, inward, landing in plans:
            @pl.when(recv)
            def _():
                inward().wait_recv()

            @pl.when(jnp.logical_not(recv))
            def _():
                landing[...] = jnp.zeros(landing.shape, f32)

        col8 = lax.broadcasted_iota(jnp.int32, (T, PACKED), 0)
        for pc in range(2):
            for i in range(R):
                for pr in range(2):
                    at = (pc * 2 + pr) * T
                    block = None
                    if i == R - 1:
                        block = row_in[p, 0, at : at + T, :]
                    if i == 0:
                        more = row_in[p, 1, at : at + T, :]
                        block = more if block is None else block + more
                    for base, at_col in ((0, T - 1), (3, 0)):
                        def pick(dg, t):
                            place_in = pc * SUB + t * 2 + pr
                            return side_in[p, base + dg + 1, place_in : place_in + 1, :]

                        line = pick(0, i + 1)
                        if i == R - 1:
                            line = line + pick(-1, 0)
                        if i == 0:
                            line = line + pick(1, R + 1)
                        more = jnp.where(col8 == at_col, line, 0.0)
                        block = more if block is None else block + more
                    at = ((pc * R + i) * 2 + pr) * T
                    hin[at : at + T, :] = block
                    hin[OWN // 2 + at : OWN // 2 + at + T, :] = block
        prec = own[...] + jnp.transpose(hin[...])

        for b in range(blocks):
            top = prec[row_of(SUB * b + SUB - 1, b) : row_of(SUB * b + SUB - 1, b) + SUB]
            last = prec[row_of(SUB * b + SUB - 2, b) : row_of(SUB * b + SUB - 2, b) + 1]
            drv[SUB * b : SUB * (b + 1), :] = jnp.where(sub < SUB - 1, top, last)
        inflate = (members - 1) / INFLATION_FACTOR
        for k in range(members):
            kb = k // SUB
            for jb in range(kb, blocks):
                out = prec[row_of(k, jb) : row_of(k, jb) + SUB]
                if jb == kb:
                    keep = {SUB - 1: sub >= SUB - 1, SUB - 2: sub >= 1}.get(k % SUB)
                    if keep is not None:
                        out = jnp.where(keep, out, 0.0)
                    out = out + jnp.where(sub == k % SUB, inflate, 0.0)
                put_entry(yfull, k, jb, out)
        for b in range(blocks):
            for e in (SUB - 1, SUB - 2):
                k = SUB * b + e
                yfull[k * members + SUB * b : k * members + SUB * (b + 1), :] = yfull[
                    pl.ds(SUB * b * members + k, SUB, stride=members), :
                ]
        squares = None
        for n in range(members * blocks):
            line = yfull[n * SUB : (n + 1) * SUB, :]
            squares = line * line if squares is None else squares + line * line
        norm = jnp.sqrt(jnp.sum(squares, axis=0, keepdims=True))
        small = 1.0 / norm
        for k in range(members):
            for jb in range(blocks):
                rows = slice(k * members + SUB * jb, k * members + SUB * (jb + 1))
                start = yfull[rows, :] * small
                first_m = -0.5 * start
                if jb == k // SUB:
                    first_m = first_m + jnp.where(sub == k % SUB, 1.5, 0.0)
                yfull[rows, :] = start
                step[rows, :] = first_m
        for kb in range(blocks):
            for r in range(quarter):
                for jb in range(blocks):
                    ypack[packed_at(kb, r, jb), :] = pack_rows(kb, r, jb, yfull)
                    zpack[packed_at(kb, r, jb), :] = pack_rows(kb, r, jb, step)
        square(ypack, step, yfull, ypack)

        def sweep(n, carry):
            square(zpack, yfull, step, None, True)
            square(ypack, step, yfull, ypack)
            square(zpack, step, zfull, zpack)
            return carry

        lax.fori_loop(0, NS_ITERS - 2, sweep, 0, unroll=True)
        square(zpack, yfull, step, None, True)
        square(zpack, step, zfull, None)

        shrink = 1.0 / jnp.sqrt(norm)

        def applied(vector):
            sums = [None] * blocks
            for i in range(members):
                lone = vector[i : i + 1, :]
                for jb in range(blocks):
                    term = lone * zfull[i * members + SUB * jb : i * members + SUB * (jb + 1), :]
                    sums[jb] = term if i == 0 else sums[jb] + term
            return [line * shrink for line in sums]

        for jb, line in enumerate(applied(drv)):
            half_ref[SUB * jb : SUB * (jb + 1), :] = line
        mean_w = applied(half_ref)
        spread = math.sqrt(members - 1) * shrink
        for k in range(members):
            for jb in range(blocks):
                wt[k, SUB * jb : SUB * (jb + 1), :] = (
                    mean_w[jb] + spread * zfull[k * members + SUB * jb : k * members + SUB * (jb + 1), :]
                )

        return carry

    def out_copy(p, away, dest, source):
        return pltpu.make_async_remote_copy(
            src_ref=outgoing.at[p, pl.ds(dest * K, K)],
            dst_ref=out_ref.at[:, :, tile(p, source), :],
            send_sem=out_send.at[p, away], recv_sem=out_recv.at[p, away],
            device_id=(dest, g), device_id_type=MESH,
        )

    wait_obs(T, m == 0)

    @pl.when(m == 0)
    def _():
        gather_seam()
        edges = []
        for i in range(R):
            products(0, i)
            edges.append(edge_weight(0, i, row_weight(0, i), 1))
        high, low = split(jnp.concatenate(edges, axis=1))
        seam = qhi[:, : R * O]
        seam_side[...] = dot(high, seam) + dot(low, seam) + dot(high, qlo[:, : R * O])

    lax.fori_loop(0, PHASES, phase, 0)
    results(PHASES - 1)

    for off in range(1, G):
        to = lax.rem(g + off, G)
        obs_copy(col_owner, to, to, col_phase, col_at).wait_send()

    @pl.when(col_owner != m)
    def _():
        obs_copy(col_owner, g, g, col_phase, col_at).wait_send()

    @pl.when(m != 0)
    def _():
        seam_copy(m).wait_send()

    for p in range(PHASES):
        for n in range(2):
            for off in range(1, M):
                ens_copy(p, n, off, lax.rem(m + off, M), m).wait_send()
        for dm, dg in near:
            send, recv, outward, inward, landing = halo_plan(p, dm, dg)

            @pl.when(send)
            def _():
                outward().wait_send()
    for p in range(PHASES):
        for off in range(1, M):
            out_copy(p, off, lax.rem(m + off, M), m).wait_send()
            out_copy(p, off, m, lax.rem(m + M - off, M)).wait_recv()


def local(M, G, ensemble, obs_value, obs_error, obs_index, obs_count):
    K, R, cols, V = ensemble.shape
    O = obs_value.shape[2]
    members = M * K
    assert cols == PHASES * M * T and cols == M * G and R == 2 and members == 24 and V == 2 * CELLS and O == LANES
    wide = T * R * O
    packed = 384
    square = members * members
    f32 = jnp.float32
    vmem = pltpu.VMEM
    dma = pltpu.SemaphoreType.DMA
    flat = lambda a: a.reshape(a.shape[0], -1)
    return pl.pallas_call(
        functools.partial(kernel, (M, G, K, R, V, O)),
        out_shape=pltpu.VMEM(ensemble.shape, f32),
        in_specs=[pl.BlockSpec(memory_space=pl.ANY)] * 4
        + [pl.BlockSpec(memory_space=pltpu.SMEM)],
        out_specs=pl.BlockSpec(memory_space=vmem),
        scratch_shapes=[
            vmem((G * R, O), f32),
            vmem((G * R, O), f32),
            vmem((G * R, O), jnp.int32),
            vmem((PHASES, members, R, T, V), f32),
            vmem((G * SUB, O), f32),
            vmem((PHASES, T * SUB, O), f32),
            vmem((R, (members + 1) * T, O), f32),
            vmem((2 * R, T, O), f32),
            vmem((TARGETS, wide), jnp.bfloat16),
            vmem((TARGETS, wide), jnp.bfloat16),
            vmem((packed, wide), jnp.bfloat16),
            vmem((packed, wide), jnp.bfloat16),
            vmem((packed, OWN), f32),
            vmem((OWN, packed), f32),
            vmem((PHASES, 2 * ROW_HALO + 2 * SIDE_HALO, packed), f32),
            vmem((PHASES, 2, ROW_HALO, packed), f32),
            vmem((PHASES, 6, SIDE_HALO, packed), f32),
            vmem((square, OWN), f32),
            vmem((square, OWN), f32),
            vmem((square, OWN), f32),
            vmem((square // 2, OWN), f32),
            vmem((square // 2, OWN), f32),
            vmem((members, OWN), f32),
            vmem((members, OWN), f32),
            vmem((members, members, OWN), f32),
            vmem((members, SUB * SUB, OWN), f32),
            vmem((SUB * SUB, OWN), f32),
            vmem((PHASES, members, R, T, V), f32),
            vmem((K, R, T, V), f32),
            vmem((V // LANES * SUB, LANES), f32),
            vmem((M * (V // LANES) * SUB, LANES), f32),
            vmem((SIDE_HALO, packed), f32),
            dma((PHASES, 2, M)), dma((PHASES, 2, M)), dma((G,)), dma((PHASES, T)),
            dma((PHASES, 9)), dma((PHASES, 9)), dma((PHASES, M)), dma((PHASES, M)), dma((4,)), dma((PHASES,)),
            pltpu.SemaphoreType.REGULAR((2,)),
            dma((1,)), dma((M,)),
        ],
        compiler_params=pltpu.CompilerParams(
            collective_id=0, has_side_effects=True, vmem_limit_bytes=56 * 1024 * 1024
        ),
    )(ensemble, flat(obs_value), flat(obs_error), flat(obs_index), obs_count.reshape(1, -1))


def solution(mesh):
    return jax.shard_map(
        functools.partial(local, mesh.shape["member"], mesh.shape["region"]),
        mesh=mesh,
        in_specs=(
            P("member", "region", None, None),
            P(None, ("member", "region"), None),
            P(None, ("member", "region"), None),
            P(None, ("member", "region"), None),
            P(None, ("member", "region")),
        ),
        out_specs=P("member", "region", None, None),
        check_vma=False,
    )
```
